32 devices in a mesh: gx: 4 (over y, core), gy: 8 (over z, x).
Axes of the slice: x: 2, y: 2, z: 4, core: 2. Of those that a mesh axis runs over, the one named last changes fastest.
Arguments:
- wavefield: float32 [8, 16, 3, 125, 256], P('gx', 'gy'), may hold values from -0.6 to 0.6
- moduli: float32 [8, 16, 2, 256], P('gx', 'gy'), may hold values from 0.5 to 4
- residuals: float32 [32, 32, 128], P(('gx', 'gy')), may hold values from -6 to 6
- coords: float32 [32, 32, 3, 128], P(('gx', 'gy')), may hold values from -1 to 1
- angles: float32 [32, 32, 2, 128], P(('gx', 'gy')), may hold values from -3.140625 to 3.140625
- element_ids: int32 [32, 32, 128], P(('gx', 'gy')), may hold values from 0 to 1023
- counts: int32 [32, 32], P(('gx', 'gy')), may hold values from 0 to 128, as said below
Outputs:
- force: float32 [8, 16, 3, 125, 256], P('gx', 'gy')
The draws below stay inside these ranges and needn't reach their ends.
Inputs may be any that keep to these rules, and one draw needn't show every extreme that they name: `counts`: each sending device has at least one tile with exactly 128 live slots; in every draw one owner receives 128 live slots from every sender. The lightest owners receive on average about a sixth of 128 a sender, the others lie between.
All inputs are finite; a program needn't handle non-finite values.
Results may differ from the reference program's by a relative error of at most 0.0003.
Values sent between devices are 32-bit elements; how exact they have to be, the bound alone decides.
A program may use at most 64 MiB of HBM per device.

```python
import math
import jax
import jax.numpy as jnp
import numpy as np
from jax import lax

CX = 2
CY = 2
EZ = 256
CAP = 128
OWNERS = 32
NXE = 8
NYE = 16
N_GX = 4
N_GY = 8


def draw_counts(key, part):
    base_key = jax.random.fold_in(key, 11)
    key_heavy, key_base, key_full = jax.random.split(base_key, 3)
    heavy = jax.random.randint(key_heavy, (OWNERS,), 1, 5)
    base = jax.random.randint(key_base, (OWNERS, OWNERS), 0, CAP // 3 + 1)
    filled = jnp.minimum(base * heavy[None, :], CAP)
    full_owner = jax.random.randint(key_full, (), 0, OWNERS)
    column = jnp.arange(OWNERS, dtype=jnp.int32)[None, :]
    return jnp.where(column == full_owner, CAP, filled).astype(jnp.int32)


def set_ends(values, stream_key, least, high):
    spot = [jax.random.randint(jax.random.fold_in(stream_key, axis), (), 0, length) for axis, length in enumerate(values.shape)]
    longest = values.shape.index(max(values.shape))
    neighbour = spot[:longest] + [(spot[longest] + 1) % values.shape[longest]] + spot[longest + 1:]
    return values.at[tuple(spot)].set(least).at[tuple(neighbour)].set(high)


def steps_of(own_key, shape, cuts, least, largest):
    factor_of, own = 1.0, jax.random.fold_in(own_key, 6)
    for axis_at, blocks in cuts:
        heights = jnp.exp(jax.random.uniform(jax.random.fold_in(own, axis_at), (blocks,), jnp.float32, least / len(cuts), largest / len(cuts)))
        factor_of = factor_of * jnp.repeat(heights, shape[axis_at] // blocks).reshape([-1 if axis == axis_at else 1 for axis in range(len(shape))])
    return factor_of


def normal_values(own_key, dims, deviation, most, pieces=(), kind=jnp.bfloat16):
    level = steps_of(own_key, dims, pieces, -0.22, 0.18) if pieces else 1.0
    drawn = jax.random.normal(own_key, dims, jnp.float32) * deviation * level
    return jnp.minimum(jnp.maximum(drawn, -most), most).astype(kind)


def setup_inputs(seed: int = 0) -> dict:
    key_of = jax.random.split(jax.random.key(seed), 8)
    wavefield = normal_values(key_of[0], (NXE, NYE, 3, 125, EZ), 0.1, 0.6, ((0, 4), (1, 8)), jnp.float32)
    moduli = jnp.clip(jnp.exp(math.log(4.0) - 2.0794415 * jax.random.uniform(key_of[1], (NXE, NYE, 2, EZ), jnp.float32) ** steps_of(key_of[1], (NXE, NYE, 2, EZ), ((0, 4), (1, 8)), -0.2, 0.2)), 0.5, 4.0)
    residuals = normal_values(key_of[2], (OWNERS, OWNERS, CAP), 1.0, 6.0, ((0, 32),), jnp.float32)
    coords = jnp.clip(jax.random.uniform(key_of[3], (OWNERS, OWNERS, 3, CAP), jnp.float32, -1.0, 1.0) * steps_of(key_of[3], (OWNERS, OWNERS, 3, CAP), ((0, 32),), -0.4, 0.0), -1.0, 1.0)
    angles = jnp.clip(jax.random.uniform(key_of[4], (OWNERS, OWNERS, 2, CAP), jnp.float32, -3.140625, 3.140625), -3.140625, 3.140625)
    element_ids = set_ends(jax.random.randint(key_of[5], (OWNERS, OWNERS, CAP), 0, CX * CY * EZ), jax.random.fold_in(key_of[5], 1), 0, (CX * CY * EZ) - 1).astype(jnp.int32)
    counts = draw_counts(jax.random.fold_in(key_of[7], 71), 0)
    return dict(wavefield=wavefield, moduli=moduli, residuals=residuals, coords=coords, angles=angles, element_ids=element_ids, counts=counts)


def gll_points():
    return np.array([-1.0, -math.sqrt(3.0 / 7.0), 0.0, math.sqrt(3.0 / 7.0), 1.0])

def gll_weights():
    return np.array([0.1, 49.0 / 90.0, 32.0 / 45.0, 49.0 / 90.0, 0.1])

def derivative_table():
    points = gll_points()
    table = np.zeros((5, 5))
    for row in range(5):
        for col in range(5):
            if row == col:
                table[row, col] = sum((1.0 / (points[col] - points[other]) for other in range(5) if other != col))
            else:
                value = 1.0 / (points[col] - points[row])
                for other in range(5):
                    if other != col and other != row:
                        value = value * (points[row] - points[other]) / (points[col] - points[other])
                table[row, col] = value
    return table

def basis(where):
    points = gll_points()
    values = []
    slopes = []
    for node in range(5):
        value = jnp.ones_like(where)
        slope = jnp.zeros_like(where)
        for other in range(5):
            if other != node:
                scale = 1.0 / (points[node] - points[other])
                factor = (where - points[other]) * scale
                slope = slope * factor + value * scale
                value = value * factor
        values.append(value)
        slopes.append(slope)
    return (jnp.stack(values), jnp.stack(slopes))

def inject(total, resid, coord, angle, ids, live_count):
    slots = resid.shape[-1]
    live = jnp.arange(slots, dtype=jnp.int32)[None, :] < live_count[:, None]
    value = jnp.where(live, resid, 0.0).reshape(-1)
    first = coord[:, 0, :].reshape(-1)
    second = coord[:, 1, :].reshape(-1)
    third = coord[:, 2, :].reshape(-1)
    azimuth = angle[:, 0, :].reshape(-1)
    dip = angle[:, 1, :].reshape(-1)
    tang_x = jnp.cos(azimuth) * jnp.cos(dip)
    tang_y = jnp.sin(azimuth) * jnp.cos(dip)
    tang_z = jnp.sin(dip)
    val_x, der_x = basis(first)
    val_y, der_y = basis(second)
    val_z, der_z = basis(third)
    shape = tang_x * der_x[:, None, None, :] * val_y[None, :, None, :] * val_z[None, None, :, :] + tang_y * val_x[:, None, None, :] * der_y[None, :, None, :] * val_z[None, None, :, :] + tang_z * val_x[:, None, None, :] * val_y[None, :, None, :] * der_z[None, None, :, :]
    direction = jnp.stack([tang_x, tang_y, tang_z]) * value[None, :]
    contrib = (direction[:, None, None, None, :] * shape[None]).reshape(375, -1)
    return total.at[:, ids.reshape(-1)].add(contrib)

def along(field, table, dim):
    if dim == 0:
        return jnp.einsum('pa,...aqsz->...pqsz', table, field, precision=lax.Precision.HIGHEST)
    if dim == 1:
        return jnp.einsum('qb,...pbsz->...pqsz', table, field, precision=lax.Precision.HIGHEST)
    return jnp.einsum('sc,...pqcz->...pqsz', table, field, precision=lax.Precision.HIGHEST)

def back(field, table, dim):
    if dim == 0:
        return jnp.einsum('pa,...pqsz->...aqsz', table, field, precision=lax.Precision.HIGHEST)
    if dim == 1:
        return jnp.einsum('qb,...pqsz->...pbsz', table, field, precision=lax.Precision.HIGHEST)
    return jnp.einsum('sc,...pqsz->...pqcz', table, field, precision=lax.Precision.HIGHEST)

def stiffness(field, moduli):
    table = jnp.asarray(derivative_table(), jnp.float32)
    weight = jnp.asarray(gll_weights(), jnp.float32)
    wgrid = (weight[:, None, None] * weight[None, :, None] * weight[None, None, :])[:, :, :, None]
    grads = [along(field, table, dim) for dim in range(3)]
    lame = moduli[..., 0, :][..., None, None, None, :]
    shear = moduli[..., 1, :][..., None, None, None, :]
    diverge = grads[0][..., 0, :, :, :, :] + grads[1][..., 1, :, :, :, :] + grads[2][..., 2, :, :, :, :]
    result = jnp.zeros_like(field)
    for col in range(3):
        parts = []
        for row in range(3):
            stress = shear * (grads[col][..., row, :, :, :, :] + grads[row][..., col, :, :, :, :])
            if row == col:
                stress = stress + lame * diverge
            parts.append(stress * wgrid)
        result = result + back(jnp.stack(parts, axis=-5), table, col)
    return result

def assemble_dim(field, e_dim, n_dim, fetch):
    count = field.shape[e_dim]
    low = lax.slice_in_dim(field, 0, 1, axis=n_dim)
    high = lax.slice_in_dim(field, 4, 5, axis=n_dim)
    middle = lax.slice_in_dim(field, 1, 4, axis=n_dim)
    first = lax.slice_in_dim(low, 0, 1, axis=e_dim)
    last = lax.slice_in_dim(high, count - 1, count, axis=e_dim)
    below, above = fetch(first, last)
    low_next = jnp.concatenate([lax.slice_in_dim(low, 1, count, axis=e_dim), above], axis=e_dim)
    high_prev = jnp.concatenate([below, lax.slice_in_dim(high, 0, count - 1, axis=e_dim)], axis=e_dim)
    return jnp.concatenate([low + high_prev, middle, high + low_next], axis=n_dim)

def fetch_none(first, last):
    return (jnp.zeros_like(last), jnp.zeros_like(first))

def reference(wavefield, moduli, residuals, coords, angles, element_ids, counts):
    owners = N_GX * N_GY
    nxe = CX * N_GX
    nye = CY * N_GY
    index = jnp.arange(owners, dtype=jnp.int32)
    owner_x = (index // N_GY)[:, None]
    owner_y = (index % N_GY)[:, None]

    def per_source(total, items):
        resid, coord, angle, ids, live_count = items
        cell_x = ids // (CY * EZ)
        cell_y = ids // EZ % CY
        cell_z = ids % EZ
        global_ids = (((owner_x * CX + cell_x) * nye + owner_y * CY + cell_y) * EZ + cell_z).astype(jnp.int32)
        return (inject(total, resid, coord, angle, global_ids, live_count), None)
    start = jnp.zeros((375, nxe * nye * EZ), jnp.float32)
    total, unused = lax.scan(per_source, start, (residuals, coords, angles, element_ids, counts))
    injected = total.reshape(3, 5, 5, 5, nxe, nye, EZ).transpose(4, 5, 0, 1, 2, 3, 6)
    field = wavefield.reshape(nxe, nye, 3, 5, 5, 5, EZ)
    internal = lax.map(lambda pair: stiffness(pair[0], pair[1]), (field, moduli))
    force = injected - internal
    force = assemble_dim(force, 0, 3, fetch_none)
    force = assemble_dim(force, 1, 4, fetch_none)
    force = assemble_dim(force, 6, 5, fetch_none)
    return force.reshape(nxe, nye, 3, 125, EZ)
```

```python
import functools
import math

import jax
import jax.numpy as jnp
import numpy as np
from jax import lax
from jax.experimental import pallas as pl
from jax.experimental.pallas import tpu as pltpu
from jax.sharding import PartitionSpec as P

MESH = pl.DeviceIdType.MESH
F32, BF16 = jnp.float32, jnp.bfloat16
PAD = 128
SPAN = 32
TILES = 4
RING, CORE = 80, 48

EDGE = [(0, 0), (0, 1), (0, 2), (0, 3), (0, 4), (1, 0), (2, 0), (3, 0)]
EDGE += [(4, 0), (4, 1), (4, 2), (4, 3), (4, 4), (1, 4), (2, 4), (3, 4)]
INNER = [(1, 1), (1, 2), (1, 3), (2, 1), (2, 2), (2, 3), (3, 1), (3, 2)]
LAST = (3, 3)


def node_order():
    order = []
    for r in range(5):
        order += [(p * 5 + q) * 5 + r for p, q in EDGE]
    for r in range(5):
        order += [(p * 5 + q) * 5 + r for p, q in INNER]
    order += [(LAST[0] * 5 + LAST[1]) * 5 + r for r in range(5)]
    return np.array(order)


def gll_points():
    return np.array([-1.0, -math.sqrt(3.0 / 7.0), 0.0, math.sqrt(3.0 / 7.0), 1.0])


def gll_weights():
    return np.array([0.1, 49.0 / 90.0, 32.0 / 45.0, 49.0 / 90.0, 0.1])


def derivative_table():
    points = gll_points()
    table = np.zeros((5, 5))
    for row in range(5):
        for col in range(5):
            if row == col:
                table[row, col] = sum(
                    (1.0 / (points[col] - points[other]) for other in range(5) if other != col)
                )
            else:
                value = 1.0 / (points[col] - points[row])
                for other in range(5):
                    if other != col and other != row:
                        value = (
                            value * (points[row] - points[other]) / (points[col] - points[other])
                        )
                table[row, col] = value
    return table


def split_table(table):
    high = table.astype(BF16)
    return high, (table - high.astype(np.float64)).astype(BF16)


def roots(k):
    points = gll_points()
    others = [m for m in range(5) if m != k]
    return [points[m] for m in others], 1.0 / np.prod([points[k] - points[m] for m in others])


def tables():
    dm, eye = derivative_table(), np.eye(5)
    w1 = gll_weights()
    weight = (w1[:, None, None] * w1[None, :, None] * w1[None, None, :]).reshape(-1)
    dirs = [
        np.kron(np.kron(dm, eye), eye),
        np.kron(np.kron(eye, dm), eye),
        np.kron(np.kron(eye, eye), dm),
    ]
    order = node_order()
    grad = np.zeros((3 * PAD, PAD))
    back = np.zeros((PAD, 3 * PAD))
    for j in range(3):
        grad[j * PAD : j * PAD + 125, :125] = dirs[j][order]
        full = -dirs[j].T * weight[None, :]
        back[:125, j * PAD : j * PAD + 125] = full[order][:, order]
    gh, gl = split_table(grad)
    bh, bl = split_table(back)
    g1 = np.concatenate([gh, gh], 1)
    bs = np.concatenate([bh, bl], 0)
    consts = np.zeros((41, 8, 128), np.float32)
    for g, group in enumerate((EDGE[:8], EDGE[8:], INNER, [LAST] * 8)):
        for row, (p, q) in enumerate(group):
            rp, sp = roots(p)
            rq, sq = roots(q)
            for j in range(4):
                consts[g * 9 + j, row] = rp[j]
                consts[g * 9 + 4 + j, row] = rq[j]
            consts[g * 9 + 8, row] = sp * sq
    for r in range(5):
        rr, sr = roots(r)
        for j in range(4):
            consts[36 + j, r] = rr[j]
        consts[40, r] = sr
    return jnp.asarray(g1), jnp.asarray(gl), jnp.asarray(bs), jnp.asarray(consts)


def split(x):
    high = x.astype(BF16)
    return high, (x - high.astype(F32)).astype(BF16)


def dot(a, b):
    return jnp.dot(a, b, preferred_element_type=F32)


def sin_cos(x):
    h = x * 0.5
    h2 = h * h
    s = c = None
    for k in range(6, -1, -1):
        a = (-1.0) ** k / math.factorial(2 * k + 1)
        b = (-1.0) ** k / math.factorial(2 * k)
        s = jnp.full(x.shape, a, F32) if s is None else s * h2 + a
        c = jnp.full(x.shape, b, F32) if c is None else c * h2 + b
    s = s * h
    return 2.0 * s * c, 1.0 - 2.0 * s * s


def quartic(x, rows):
    a, b, c, d = [x - row for row in rows]
    ab, cd = a * b, c * d
    return ab * cd, (a + b) * cd + ab * (c + d)


def moves_of(cx, cy):
    moves = [(2 * s - 1, 0) for s in (0, 1)] + [(0, 2 * s - 1) for s in (0, 1)]
    moves += [(2 * x - 1, 2 * y - 1) for x in (0, 1) for y in (0, 1)]
    return moves


OPPOSITE = [1, 0, 3, 2, 7, 6, 5, 4]


def neighbour(m, gx, gy, nx, ny, cx, cy):
    ok = None
    for pos, step, total in ((gx, moves_of(cx, cy)[m][0], nx), (gy, moves_of(cx, cy)[m][1], ny)):
        if step:
            c = pos > 0 if step < 0 else pos < total - 1
            ok = c if ok is None else ok & c
    return ok


def step_kernel(
    nx, ny, cx, cy, resid_h, coord_h, angle_h, ids_h, count_h, u_h, mod_h, g1_h, g2_h, bs_h,
    consts_h, pre_h, rx, ry, rc,
    resid, coord, angle, ids, count, u_ref, mod_ref, g1, g2, bs, consts, pre,
    packed, got, acc, lhs_a, lhs_b, in_a, in_b, hot_a, hot_b, pad, xs, ys, cs,
    load_sem, store_sem, send_sem, recv_sem, halo_send, halo_recv,
):
    n = nx * ny
    gx, gy = lax.axis_index("gx"), lax.axis_index("gy")
    me = gx * ny + gy
    cells, depth, slots = cx * cy, acc.shape[2], resid.shape[2]
    halves = depth // 128
    rows_node = halves * cy
    span = min(n, SPAN)
    chunks = span // TILES
    width = TILES * slots
    barrier = pltpu.get_barrier_semaphore()

    def greet(k, c):
        to = lax.rem(me + k, n)
        pl.semaphore_signal(
            barrier, inc=1, device_id=(to // ny, lax.rem(to, ny)), device_id_type=MESH
        )
        return c

    pairs = [
        (count_h, count), (angle_h, angle), (resid_h, resid), (coord_h, coord), (ids_h, ids),
        (u_h, u_ref), (mod_h, mod_ref), (g1_h, g1), (g2_h, g2), (bs_h, bs), (consts_h, consts),
    ]
    loads = [pltpu.make_async_copy(a, b, load_sem.at[k]) for k, (a, b) in enumerate(pairs)]
    for copy in loads:
        copy.start()
    lax.fori_loop(1, n, greet, 0)
    for copy in loads[:5]:
        copy.wait()

    rows = lax.broadcasted_iota(jnp.int32, (n, n), 0)
    cols = lax.broadcasted_iota(jnp.int32, (n, n), 1)
    diagonal = jnp.where(rows == cols, count[...].astype(F32), 0.0)
    live_count = jnp.sum(diagonal, axis=1, keepdims=True)
    slot = lax.broadcasted_iota(jnp.int32, (n, slots), 1).astype(F32)
    sa, ca = sin_cos(angle[0, :, 0, :])
    sd, cd = sin_cos(angle[0, :, 1, :])
    packed[:, 0, :] = jnp.where(slot < live_count, resid[0], 0.0)
    for d in range(3):
        packed[:, 1 + d, :] = coord[0, d]
    packed[:, 4, :] = ca * cd
    packed[:, 5, :] = sa * cd
    packed[:, 6, :] = sd
    packed[:, 7, :] = ids[0].astype(F32)
    pl.semaphore_wait(barrier, n - 1)

    def tile_copy(k, to, at):
        return pltpu.make_async_remote_copy(
            src_ref=packed.at[to],
            dst_ref=got.at[at],
            send_sem=send_sem.at[k],
            recv_sem=recv_sem.at[k],
            device_id=(to // ny, lax.rem(to, ny)),
            device_id_type=MESH,
        )

    def send(k, c):
        tile_copy(k, lax.rem(me + k, n), me).start()
        return c

    lax.fori_loop(1, n, send, 0)
    got[me] = packed[me]
    pad[...] = jnp.zeros_like(pad)
    for copy in loads[5:]:
        copy.wait()

    def stiff(cell, slab):
        g = []
        for c in range(3):
            start = ((cell // cy) * 3 + c) * 125 * rows_node + cell % cy
            for h in range(halves):
                pad[slab, c, 0:125, h * 128 : (h + 1) * 128] = u_ref[
                    pl.ds(start + h * cy, 125, stride=rows_node), :
                ]
            high, low = split(pad[slab, c])
            r = dot(g1[...], jnp.concatenate([high, low], axis=0)) + dot(g2[...], high)
            g.append([r[j * PAD : (j + 1) * PAD] for j in range(3)])
        lam, mu = mod_ref[cell, 0:1, :], mod_ref[cell, 1:2, :]
        press = lam * (g[0][0] + g[1][1] + g[2][2])
        for i in range(3):
            parts = []
            for j in range(3):
                s = mu * (g[i][j] + g[j][i])
                parts.append(s + press if i == j else s)
            high, low = split(jnp.concatenate(parts, axis=0))
            r = dot(bs[...], high)
            acc[cell, i * PAD : (i + 1) * PAD, :] = r[:PAD] + r[PAD:] + dot(bs[:PAD], low)

    for cell in range(cells):
        stiff(cell, cell % 2)

    def wait_tile(k):
        tile_copy(k, lax.rem(me + k, n), lax.rem(me - k + n, n)).wait_recv()

    def prepare(first, ring, inner, hot, at):
        tiles = [got[lax.rem(me - (first + i) + n, n)] for i in range(TILES)]
        tile = jnp.concatenate(tiles, axis=1)

        def const(k):
            return jnp.concatenate([consts[k]] * TILES, axis=1)

        v = tile[0:1]
        t = [tile[4 + i : 5 + i] for i in range(3)]
        x, y, z = [jnp.broadcast_to(tile[1 + d : 2 + d], (8, width)) for d in range(3)]
        lz, dz = quartic(z, [const(36 + j) for j in range(4)])
        lz, dz = lz * const(40), dz * (const(40) * t[2])
        first_of, second_of = [], []
        for g in range(4):
            lx, dx = quartic(x, [const(g * 9 + j) for j in range(4)])
            ly, dy = quartic(y, [const(g * 9 + 4 + j) for j in range(4)])
            scale = const(g * 9 + 8)
            first_of.append(scale * ((t[0] * dx) * ly + (t[1] * dy) * lx))
            second_of.append(scale * (lx * ly))
        edge, core = [], []
        for r in range(5):
            a = jnp.broadcast_to(lz[r : r + 1], (8, width))
            b = jnp.broadcast_to(dz[r : r + 1], (8, width))
            edge += [first_of[g] * a + second_of[g] * b for g in (0, 1)]
            core.append(first_of[2] * a + second_of[2] * b)
        core.append(first_of[3] * lz + second_of[3] * dz)
        edge, core = jnp.concatenate(edge, axis=0), jnp.concatenate(core, axis=0)
        for i in range(3):
            w = v * t[i]
            high, low = split(edge * w)
            ring[2 * i * RING : (2 * i + 1) * RING, :] = high
            ring[(2 * i + 1) * RING : (2 * i + 2) * RING, :] = low
            high, low = split(core * w)
            inner[2 * i * CORE : (2 * i + 1) * CORE, pl.ds(at, width)] = high
            inner[(2 * i + 1) * CORE : (2 * i + 2) * CORE, pl.ds(at, width)] = low
        number = lax.broadcasted_iota(jnp.int32, (slots, cells * depth), 1).astype(F32)
        for i in range(TILES):
            ident = tiles[i].T[:, 7:8]
            hot[pl.ds(at + i * slots, slots), :] = jnp.where(number == ident, 1.0, 0.0).astype(BF16)

    def gather_ring(ring, hot, at):
        for cell in range(cells):
            r = dot(ring[...], hot[pl.ds(at, width), cell * depth : (cell + 1) * depth])
            for i in range(3):
                acc[cell, i * PAD : i * PAD + RING, :] += (
                    r[2 * i * RING : (2 * i + 1) * RING]
                    + r[(2 * i + 1) * RING : (2 * i + 2) * RING]
                )

    def gather_core(cell):
        where = slice(cell * depth, (cell + 1) * depth)
        r = dot(in_a[...], hot_a[:, where]) + dot(in_b[...], hot_b[:, where])
        return [
            acc[cell, i * PAD + RING : (i + 1) * PAD, :]
            + r[2 * i * CORE : (2 * i + 1) * CORE]
            + r[(2 * i + 1) * CORE : (2 * i + 2) * CORE]
            for i in range(3)
        ]

    def inject(first, last):
        for i in range(TILES):
            wait_tile(first + i)
        prepare(first, lhs_a, in_a, hot_a, 0)

        def pair(j, carry):
            one, two = first + (2 * j + 1) * TILES, first + (2 * j + 2) * TILES
            for i in range(2 * TILES):
                wait_tile(one + i)
            here = pl.multiple_of(j * width, width)
            then = pl.multiple_of((j + 1) * width, width)
            prepare(one, lhs_b, in_b, hot_b, here)
            gather_ring(lhs_a, hot_a, here)
            prepare(two, lhs_a, in_a, hot_a, then)
            gather_ring(lhs_b, hot_b, here)
            return carry

        half = chunks // 2
        lax.fori_loop(0, half - 1, pair, 0)
        end = first + (chunks - 1) * TILES
        for i in range(TILES - 1 if last else TILES):
            wait_tile(end + i)
        prepare(end, lhs_b, in_b, hot_b, (half - 1) * width)
        gather_ring(lhs_a, hot_a, (half - 1) * width)
        gather_ring(lhs_b, hot_b, (half - 1) * width)

    if n > span:
        def early(b, carry):
            inject(b * span + 1, False)
            for cell in range(cells):
                for i, f in enumerate(gather_core(cell)):
                    acc[cell, i * PAD + RING : (i + 1) * PAD, :] = f
            return carry

        lax.fori_loop(0, n // span - 1, early, 0)
    inject(n - span + 1, True)

    def stitch(low, high):
        lane = lax.broadcasted_iota(jnp.int32, low.shape, 1)
        up = jnp.where(lane < depth - 1, pltpu.roll(low, depth - 1, 1), 0.0)
        down = jnp.where(lane > 0, pltpu.roll(high, 1, 1), 0.0)
        return low + down, high + up

    def join(a, ra, b, rb, size):
        total = acc[a, ra : ra + size, :] + acc[b, rb : rb + size, :]
        acc[a, ra : ra + size, :] = total
        acc[b, rb : rb + size, :] = total

    moves = moves_of(cx, cy)

    def there(m):
        return neighbour(m, gx, gy, nx, ny, cx, cy)

    def strip_copy(c, m, sem, mine, theirs):
        src, dst = ((xs, rx), (ys, ry), (cs, rc))[(m >= 2) + (m >= 4)]
        dx, dy = moves[m]
        return pltpu.make_async_remote_copy(
            src_ref=src.at[(c,) + mine],
            dst_ref=dst.at[(c,) + theirs],
            send_sem=halo_send.at[c * 8 + m],
            recv_sem=halo_recv.at[c * 8 + sem],
            device_id=(gx + dx, gy + dy),
            device_id_type=MESH,
        )

    def place(m):
        return (m % 2,) if m < 4 else ((m - 4) // 2, m % 2)

    def outgoing(c, m):
        return strip_copy(c, m, m, place(m), place(OPPOSITE[m]))

    def incoming(c, m):
        return strip_copy(c, m, OPPOSITE[m], place(m), place(m))

    for c in range(3):
        o = c * PAD
        for cell in range(cells):
            low, high = stitch(acc[cell, o : o + 16, :], acc[cell, o + 64 : o + 80, :])
            acc[cell, o : o + 16, :] = low
            acc[cell, o + 64 : o + 80, :] = high
        for r in range(5):
            k = o + r * 16
            for y in range(cy):
                for x in range(cx - 1):
                    join(x * cy + y, k + 8, (x + 1) * cy + y, k, 5)
            for x in range(cx):
                for y in range(cy - 1):
                    a, b = x * cy + y, x * cy + y + 1
                    join(a, k + 13, b, k + 5, 3)
                    join(a, k + 4, b, k, 1)
                    join(a, k + 12, b, k + 8, 1)
        for x in range(cx):
            for side in (0, 1):
                cell = x * cy + side * (cy - 1)
                for h in range(halves):
                    lanes = slice(h * 128, (h + 1) * 128)
                    for r in range(5):
                        k = o + r * 16
                        low, mid, high = ((0, 5, 8), (4, 13, 12))[side]
                        to = x * 25 * halves + r * halves + h
                        step = 5 * halves
                        ys[c, side, to : to + 1, :] = acc[cell, k + low : k + low + 1, lanes]
                        ys[c, side, pl.ds(to + step, 3, stride=step), :] = acc[
                            cell, k + mid : k + mid + 3, lanes
                        ]
                        ys[c, side, to + 4 * step : to + 4 * step + 1, :] = acc[
                            cell, k + high : k + high + 1, lanes
                        ]
        for m in (2, 3):
            @pl.when(there(m))
            def _():
                outgoing(c, m).start()
        for y in range(cy):
            for side in (0, 1):
                cell = side * (cx - 1) * cy + y
                for h in range(halves):
                    for r in range(5):
                        k = o + r * 16 + side * 8
                        xs[c, side, pl.ds(r * rows_node + h * cy + y, 5, stride=5 * rows_node), :] = (
                            acc[cell, k : k + 5, h * 128 : (h + 1) * 128]
                        )
        for x in (0, 1):
            for y in (0, 1):
                cell = x * (cx - 1) * cy + y * (cy - 1)
                for h in range(halves):
                    for r in range(5):
                        k = o + r * 16 + x * 8 + y * 4
                        cs[c, x, y, r * halves + h : r * halves + h + 1, :] = acc[
                            cell, k : k + 1, h * 128 : (h + 1) * 128
                        ]
        for m in (0, 1, 4, 5, 6, 7):
            @pl.when(there(m))
            def _():
                outgoing(c, m).start()

    def place_rows(cell, c, values, row, size, node, step):
        start = ((cell // cy) * 3 + c) * 125 * rows_node + cell % cy
        for h in range(halves):
            at = start + h * cy + node * rows_node
            part = values[row : row + size, h * 128 : (h + 1) * 128]
            pre[pl.ds(at, size, stride=step * rows_node), :] = part

    stores = []
    done = 0
    for x in range(cx):
        for y in range(cy):
            cell = x * cy + y
            inner = gather_core(cell)
            for c in range(3):
                f = inner[c]
                low, high = stitch(f[0:8], f[32:40])
                lane = lax.broadcasted_iota(jnp.int32, (8, depth), 1)
                row = lax.broadcasted_iota(jnp.int32, (8, depth), 0)
                tail = f[40:48]
                up = pltpu.roll(pltpu.roll(tail, depth - 1, 1), 4, 0)
                down = pltpu.roll(pltpu.roll(tail, 1, 1), 4, 0)
                tail = (
                    tail
                    + jnp.where((row == 4) & (lane < depth - 1), up, 0.0)
                    + jnp.where((row == 0) & (lane > 0), down, 0.0)
                )
                planes = [low, f[8:16], f[16:24], f[24:32], high]
                for r in range(5):
                    ring = acc[cell, c * PAD + r * 16 : c * PAD + r * 16 + 16, :]
                    place_rows(cell, c, ring, 0, 5, r, 5)
                    place_rows(cell, c, ring, 5, 3, 25 + r, 25)
                    place_rows(cell, c, ring, 8, 5, 100 + r, 5)
                    place_rows(cell, c, ring, 13, 3, 45 + r, 25)
                    place_rows(cell, c, planes[r], 0, 3, 30 + r, 5)
                    place_rows(cell, c, planes[r], 3, 3, 55 + r, 5)
                    place_rows(cell, c, planes[r], 6, 2, 80 + r, 5)
                place_rows(cell, c, tail, 0, 5, 90, 1)
        for c in range(3):
            upto = (x * 3 + c + 1) * 125 * rows_node // 8 * 8
            copy = pltpu.make_async_copy(
                pre.at[pl.ds(done, upto - done)],
                pre_h.at[pl.ds(done, upto - done)],
                store_sem.at[x * 3 + c],
            )
            copy.start()
            stores.append(copy)
            done = upto

    def drain(k, c):
        tile_copy(k, lax.rem(me + k, n), me).wait_send()
        return c

    lax.fori_loop(1, n, drain, 0)
    for c in range(3):
        for m in range(8):
            @pl.when(there(m))
            def _():
                incoming(c, m).wait_recv()
                outgoing(c, m).wait_send()
    for copy in stores:
        copy.wait()


def finish_kernel(
    nx, ny, cx, cy, pre_h, rx_h, ry_h, rc_h, out_h, buf, bx, by, bc, load_sem, strip_sem, out_sem
):
    gx, gy = lax.axis_index("gx"), lax.axis_index("gy")
    total = buf.shape[0]
    block = total // (cx * 3)
    rows_node = block // 125
    halves = rows_node // cy

    def strip(m):
        src, dst = ((rx_h, bx), (ry_h, by), (rc_h, bc))[(m >= 2) + (m >= 4)]
        at = (m % 2,) if m < 4 else ((m - 4) // 2, m % 2)
        where = (slice(None),) + at
        return pltpu.make_async_copy(src.at[where], dst.at[where], strip_sem.at[m]), dst, where

    def there(m):
        return neighbour(m, gx, gy, nx, ny, cx, cy)

    for m in range(8):
        copy, dst, where = strip(m)

        @pl.when(there(m))
        def _():
            copy.start()

        @pl.when(jnp.logical_not(there(m)))
        def _():
            hole = dst.at[where]
            hole[...] = jnp.zeros(hole.shape, F32)

    loads, done = [], 0
    for k in range(cx * 3):
        upto = min(-(-(k + 1) * block // 8) * 8, total)
        copy = pltpu.make_async_copy(
            pre_h.at[pl.ds(done, upto - done)], buf.at[pl.ds(done, upto - done)], load_sem.at[k]
        )
        copy.start()
        loads.append(copy)
        done = upto
    for m in range(8):
        copy, dst, where = strip(m)

        @pl.when(there(m))
        def _():
            copy.wait()

    stores, done = [], 0
    for k in range(cx * 3):
        x, c = k // 3, k % 3
        loads[k].wait()
        base = k * block
        face = 25 * rows_node
        if x == 0:
            buf[base : base + face, :] += bx[c, 0]
        if x == cx - 1:
            buf[base + 4 * face : base + 5 * face, :] += bx[c, 1]
        line = 5 * halves
        for side in (0, 1):
            y = side * (cy - 1)
            for p in range(5):
                at = base + (p * 25 + side * 20) * rows_node + y
                where = pl.ds(at, line, stride=cy)
                k0 = (x * 5 + p) * line
                add = by[c, side, k0 : k0 + line, :]
                if x == 0 and p == 0:
                    add = add + bc[c, 0, side]
                if x == cx - 1 and p == 4:
                    add = add + bc[c, 1, side]
                buf[where, :] += add
        upto = (k + 1) * block // 8 * 8
        copy = pltpu.make_async_copy(
            buf.at[pl.ds(done, upto - done)], out_h.at[pl.ds(done, upto - done)], out_sem.at[k]
        )
        copy.start()
        stores.append(copy)
        done = upto
    for copy in stores:
        copy.wait()


def anywhere(count):
    return [pl.BlockSpec(memory_space=pl.ANY)] * count


def body(nx, ny, wavefield, moduli, residuals, coords, angles, element_ids, counts):
    cx, cy, depth = wavefield.shape[0], wavefield.shape[1], wavefield.shape[4]
    n, slots = nx * ny, residuals.shape[2]
    cells, halves = cx * cy, depth // 128
    span = min(n, SPAN)
    width = TILES * slots
    rows = wavefield.transpose(0, 2, 3, 1, 4).reshape(cx, 3, 125, cy, halves, 128)
    rows = rows.transpose(0, 1, 2, 4, 3, 5).reshape(-1, 128)
    coords = coords.transpose(0, 2, 1, 3)
    moduli = moduli.reshape(cells, 2, depth)
    operands = [residuals, coords, angles, element_ids, counts, rows, moduli, *tables()]
    strips = [
        (3, 2, 25 * halves * cy, 128),
        (3, 2, cx * 25 * halves, 128),
        (3, 2, 2, 5 * halves, 128),
    ]
    scratch = [pltpu.VMEM(a.shape, a.dtype) for a in operands]
    scratch += [
        pltpu.VMEM(rows.shape, F32),
        pltpu.VMEM((n, 8, slots), F32),
        pltpu.VMEM((n, 8, slots), F32),
        pltpu.VMEM((cells, 3 * PAD, depth), F32),
        pltpu.VMEM((6 * RING, width), BF16),
        pltpu.VMEM((6 * RING, width), BF16),
        pltpu.VMEM((6 * CORE, span * slots // 2), BF16),
        pltpu.VMEM((6 * CORE, span * slots // 2), BF16),
        pltpu.VMEM((span * slots // 2, cells * depth), BF16),
        pltpu.VMEM((span * slots // 2, cells * depth), BF16),
        pltpu.VMEM((2, 3, PAD, depth), F32),
    ]
    scratch += [pltpu.VMEM(s, F32) for s in strips]
    scratch += [
        pltpu.SemaphoreType.DMA((len(operands),)),
        pltpu.SemaphoreType.DMA((cx * 3,)),
        pltpu.SemaphoreType.DMA((n,)),
        pltpu.SemaphoreType.DMA((n,)),
        pltpu.SemaphoreType.DMA((24,)),
        pltpu.SemaphoreType.DMA((24,)),
    ]
    parts = pl.pallas_call(
        functools.partial(step_kernel, nx, ny, cx, cy),
        out_shape=[jax.ShapeDtypeStruct(s, F32) for s in [rows.shape] + strips],
        in_specs=anywhere(len(operands)),
        out_specs=anywhere(4),
        scratch_shapes=scratch,
        compiler_params=pltpu.CompilerParams(collective_id=0, has_side_effects=True),
    )(*operands)
    force = pl.pallas_call(
        functools.partial(finish_kernel, nx, ny, cx, cy),
        out_shape=jax.ShapeDtypeStruct(rows.shape, F32),
        in_specs=anywhere(4),
        out_specs=anywhere(1)[0],
        scratch_shapes=[pltpu.VMEM(s, F32) for s in [rows.shape] + strips]
        + [
            pltpu.SemaphoreType.DMA((cx * 3,)),
            pltpu.SemaphoreType.DMA((8,)),
            pltpu.SemaphoreType.DMA((cx * 3,)),
        ],
    )(*parts)
    force = force.reshape(cx, 3, 125, halves, cy, 128).transpose(0, 1, 2, 4, 3, 5)
    return force.reshape(cx, 3, 125, cy, depth).transpose(0, 3, 1, 2, 4)


def solution(mesh):
    in_specs = (
        P("gx", "gy", None, None, None),
        P("gx", "gy", None, None),
        P(("gx", "gy"), None, None),
        P(("gx", "gy"), None, None, None),
        P(("gx", "gy"), None, None, None),
        P(("gx", "gy"), None, None),
        P(("gx", "gy"), None),
    )
    out_specs = P("gx", "gy", None, None, None)
    return jax.shard_map(
        functools.partial(body, mesh.shape["gx"], mesh.shape["gy"]),
        mesh=mesh,
        in_specs=in_specs,
        out_specs=out_specs,
        check_vma=False,
    )
```

```python
import functools
import math

import jax
import jax.numpy as jnp
import numpy as np
from jax import lax
from jax.experimental import pallas as pl
from jax.experimental.pallas import tpu as pltpu
from jax.sharding import PartitionSpec as P

MESH = pl.DeviceIdType.MESH
F32, BF16 = jnp.float32, jnp.bfloat16
PAD = 128
SPAN = 32
TILES = 4
RING, CORE = 80, 48

EDGE = [(0, 0), (0, 1), (0, 2), (0, 3), (0, 4), (1, 0), (2, 0), (3, 0)]
EDGE += [(4, 0), (4, 1), (4, 2), (4, 3), (4, 4), (1, 4), (2, 4), (3, 4)]
INNER = [(1, 1), (1, 2), (1, 3), (2, 1), (2, 2), (2, 3), (3, 1), (3, 2)]
LAST = (3, 3)


def node_order():
    order = []
    for r in range(5):
        order += [(p * 5 + q) * 5 + r for p, q in EDGE]
    for r in range(5):
        order += [(p * 5 + q) * 5 + r for p, q in INNER]
    order += [(LAST[0] * 5 + LAST[1]) * 5 + r for r in range(5)]
    return np.array(order)


def gll_points():
    return np.array([-1.0, -math.sqrt(3.0 / 7.0), 0.0, math.sqrt(3.0 / 7.0), 1.0])


def gll_weights():
    return np.array([0.1, 49.0 / 90.0, 32.0 / 45.0, 49.0 / 90.0, 0.1])


def derivative_table():
    points = gll_points()
    table = np.zeros((5, 5))
    for row in range(5):
        for col in range(5):
            if row == col:
                table[row, col] = sum(
                    (1.0 / (points[col] - points[other]) for other in range(5) if other != col)
                )
            else:
                value = 1.0 / (points[col] - points[row])
                for other in range(5):
                    if other != col and other != row:
                        value = (
                            value * (points[row] - points[other]) / (points[col] - points[other])
                        )
                table[row, col] = value
    return table


def split_table(table):
    high = table.astype(BF16)
    return high, (table - high.astype(np.float64)).astype(BF16)


def roots(k):
    points = gll_points()
    others = [m for m in range(5) if m != k]
    return [points[m] for m in others], 1.0 / np.prod([points[k] - points[m] for m in others])


def tables():
    dm, eye = derivative_table(), np.eye(5)
    w1 = gll_weights()
    weight = (w1[:, None, None] * w1[None, :, None] * w1[None, None, :]).reshape(-1)
    dirs = [
        np.kron(np.kron(dm, eye), eye),
        np.kron(np.kron(eye, dm), eye),
        np.kron(np.kron(eye, eye), dm),
    ]
    order = node_order()
    grad = np.zeros((3 * PAD, PAD))
    back = np.zeros((PAD, 3 * PAD))
    for j in range(3):
        grad[j * PAD : j * PAD + 125, :125] = dirs[j][order]
        full = -dirs[j].T * weight[None, :]
        back[:125, j * PAD : j * PAD + 125] = full[order][:, order]
    gh, gl = split_table(grad)
    bh, bl = split_table(back)
    g1 = np.concatenate([gh, gh], 1)
    bs = np.concatenate([bh, bl], 0)
    consts = np.zeros((41, 8, 128), np.float32)
    for g, group in enumerate((EDGE[:8], EDGE[8:], INNER, [LAST] * 8)):
        for row, (p, q) in enumerate(group):
            rp, sp = roots(p)
            rq, sq = roots(q)
            for j in range(4):
                consts[g * 9 + j, row] = rp[j]
                consts[g * 9 + 4 + j, row] = rq[j]
            consts[g * 9 + 8, row] = sp * sq
    for r in range(5):
        rr, sr = roots(r)
        for j in range(4):
            consts[36 + j, r] = rr[j]
        consts[40, r] = sr
    return jnp.asarray(g1), jnp.asarray(gl), jnp.asarray(bs), jnp.asarray(consts)


def split(x):
    high = x.astype(BF16)
    return high, (x - high.astype(F32)).astype(BF16)


def dot(a, b):
    return jnp.dot(a, b, preferred_element_type=F32)


def sin_cos(x):
    h = x * 0.5
    h2 = h * h
    s = c = None
    for k in range(6, -1, -1):
        a = (-1.0) ** k / math.factorial(2 * k + 1)
        b = (-1.0) ** k / math.factorial(2 * k)
        s = jnp.full(x.shape, a, F32) if s is None else s * h2 + a
        c = jnp.full(x.shape, b, F32) if c is None else c * h2 + b
    s = s * h
    return 2.0 * s * c, 1.0 - 2.0 * s * s


def quartic(x, rows):
    a, b, c, d = [x - row for row in rows]
    ab, cd = a * b, c * d
    return ab * cd, (a + b) * cd + ab * (c + d)


MOVES = [(-1, 0), (1, 0), (0, -1), (0, 1)]


def neighbour(m, gx, gy, nx, ny):
    step = MOVES[m][m // 2]
    pos, total = ((gx, nx), (gy, ny))[m // 2]
    return pos > 0 if step < 0 else pos < total - 1


def step_kernel(
    nx, ny, cx, cy, resid_h, coord_h, angle_h, ids_h, count_h, u_h, mod_h, g1_h, g2_h, bs_h,
    consts_h, pre_h, rx, ry, re,
    resid, coord, angle, ids, count, u_ref, mod_ref, g1, g2, bs, consts,
    packed, got, acc, lhs_a, lhs_b, in_a, in_b, hot_a, hot_b, pad, xs, ys, es, tips,
    load_sem, send_sem, recv_sem, halo_send, halo_recv,
):
    n = nx * ny
    gx, gy = lax.axis_index("gx"), lax.axis_index("gy")
    me = gx * ny + gy
    cells, depth, slots = cx * cy, acc.shape[2], resid.shape[2]
    halves = depth // 128
    rows_node = halves * cy
    span = min(n, SPAN)
    chunks = span // TILES
    width = TILES * slots
    barrier = pltpu.get_barrier_semaphore()

    def greet(k, c):
        to = lax.rem(me + k, n)
        pl.semaphore_signal(
            barrier, inc=1, device_id=(to // ny, lax.rem(to, ny)), device_id_type=MESH
        )
        return c

    pairs = [
        (count_h, count), (angle_h, angle), (resid_h, resid), (coord_h, coord), (ids_h, ids),
        (u_h, u_ref), (mod_h, mod_ref), (g1_h, g1), (g2_h, g2), (bs_h, bs), (consts_h, consts),
    ]
    loads = [pltpu.make_async_copy(a, b, load_sem.at[k]) for k, (a, b) in enumerate(pairs)]
    for copy in loads:
        copy.start()
    lax.fori_loop(1, n, greet, 0)
    for copy in loads[:5]:
        copy.wait()

    rows = lax.broadcasted_iota(jnp.int32, (n, n), 0)
    cols = lax.broadcasted_iota(jnp.int32, (n, n), 1)
    diagonal = jnp.where(rows == cols, count[...].astype(F32), 0.0)
    live_count = jnp.sum(diagonal, axis=1, keepdims=True)
    slot = lax.broadcasted_iota(jnp.int32, (n, slots), 1).astype(F32)
    sa, ca = sin_cos(angle[0, :, 0, :])
    sd, cd = sin_cos(angle[0, :, 1, :])
    packed[:, 0, :] = jnp.where(slot < live_count, resid[0], 0.0)
    for d in range(3):
        packed[:, 1 + d, :] = coord[0, d]
    packed[:, 4, :] = ca * cd
    packed[:, 5, :] = sa * cd
    packed[:, 6, :] = sd
    packed[:, 7, :] = ids[0].astype(F32)
    tips[...] = jnp.zeros_like(tips)
    for m in range(4):
        @pl.when(jnp.logical_not(neighbour(m, gx, gy, nx, ny)))
        def _():
            for hole in ((rx,), (ry, re))[m // 2]:
                hole[m % 2] = jnp.zeros(hole.shape[1:], F32)

    pl.semaphore_wait(barrier, n - 1)

    def tile_copy(k, to, at):
        return pltpu.make_async_remote_copy(
            src_ref=packed.at[to],
            dst_ref=got.at[at],
            send_sem=send_sem.at[k],
            recv_sem=recv_sem.at[k],
            device_id=(to // ny, lax.rem(to, ny)),
            device_id_type=MESH,
        )

    def send(k, c):
        tile_copy(k, lax.rem(me + k, n), me).start()
        return c

    lax.fori_loop(1, n, send, 0)
    got[me] = packed[me]
    pad[...] = jnp.zeros_like(pad)
    for copy in loads[5:]:
        copy.wait()

    def stiff(cell, slab):
        g = []
        for c in range(3):
            start = ((cell // cy) * 3 + c) * 125 * rows_node + cell % cy
            for h in range(halves):
                pad[slab, c, 0:125, h * 128 : (h + 1) * 128] = u_ref[
                    pl.ds(start + h * cy, 125, stride=rows_node), :
                ]
            high, low = split(pad[slab, c])
            r = dot(g1[...], jnp.concatenate([high, low], axis=0)) + dot(g2[...], high)
            g.append([r[j * PAD : (j + 1) * PAD] for j in range(3)])
        lam, mu = mod_ref[cell, 0:1, :], mod_ref[cell, 1:2, :]
        press = lam * (g[0][0] + g[1][1] + g[2][2])
        for i in range(3):
            parts = []
            for j in range(3):
                s = mu * (g[i][j] + g[j][i])
                parts.append(s + press if i == j else s)
            high, low = split(jnp.concatenate(parts, axis=0))
            r = dot(bs[...], high)
            acc[cell, i * PAD : (i + 1) * PAD, :] = r[:PAD] + r[PAD:] + dot(bs[:PAD], low)

    for cell in range(cells):
        stiff(cell, cell % 2)

    def wait_tile(k):
        tile_copy(k, lax.rem(me + k, n), lax.rem(me - k + n, n)).wait_recv()

    def prepare(first, ring, inner, hot, at):
        tiles = [got[lax.rem(me - (first + i) + n, n)] for i in range(TILES)]
        tile = jnp.concatenate(tiles, axis=1)

        def const(k):
            return jnp.concatenate([consts[k]] * TILES, axis=1)

        v = tile[0:1]
        t = [tile[4 + i : 5 + i] for i in range(3)]
        x, y, z = [jnp.broadcast_to(tile[1 + d : 2 + d], (8, width)) for d in range(3)]
        lz, dz = quartic(z, [const(36 + j) for j in range(4)])
        lz, dz = lz * const(40), dz * (const(40) * t[2])
        first_of, second_of = [], []
        for g in range(4):
            lx, dx = quartic(x, [const(g * 9 + j) for j in range(4)])
            ly, dy = quartic(y, [const(g * 9 + 4 + j) for j in range(4)])
            scale = const(g * 9 + 8)
            first_of.append(scale * ((t[0] * dx) * ly + (t[1] * dy) * lx))
            second_of.append(scale * (lx * ly))
        edge, core = [], []
        for r in range(5):
            a = jnp.broadcast_to(lz[r : r + 1], (8, width))
            b = jnp.broadcast_to(dz[r : r + 1], (8, width))
            edge += [first_of[g] * a + second_of[g] * b for g in (0, 1)]
            core.append(first_of[2] * a + second_of[2] * b)
        core.append(first_of[3] * lz + second_of[3] * dz)
        edge, core = jnp.concatenate(edge, axis=0), jnp.concatenate(core, axis=0)
        for i in range(3):
            w = v * t[i]
            high, low = split(edge * w)
            ring[2 * i * RING : (2 * i + 1) * RING, :] = high
            ring[(2 * i + 1) * RING : (2 * i + 2) * RING, :] = low
            high, low = split(core * w)
            inner[2 * i * CORE : (2 * i + 1) * CORE, pl.ds(at, width)] = high
            inner[(2 * i + 1) * CORE : (2 * i + 2) * CORE, pl.ds(at, width)] = low
        number = lax.broadcasted_iota(jnp.int32, (slots, cells * depth), 1).astype(F32)
        for i in range(TILES):
            ident = tiles[i].T[:, 7:8]
            hot[pl.ds(at + i * slots, slots), :] = jnp.where(number == ident, 1.0, 0.0).astype(BF16)

    def gather_ring(ring, hot, at):
        for cell in range(cells):
            r = dot(ring[...], hot[pl.ds(at, width), cell * depth : (cell + 1) * depth])
            for i in range(3):
                acc[cell, i * PAD : i * PAD + RING, :] += (
                    r[2 * i * RING : (2 * i + 1) * RING]
                    + r[(2 * i + 1) * RING : (2 * i + 2) * RING]
                )

    def gather_core(cell):
        where = slice(cell * depth, (cell + 1) * depth)
        r = dot(in_a[...], hot_a[:, where]) + dot(in_b[...], hot_b[:, where])
        return [
            acc[cell, i * PAD + RING : (i + 1) * PAD, :]
            + r[2 * i * CORE : (2 * i + 1) * CORE]
            + r[(2 * i + 1) * CORE : (2 * i + 2) * CORE]
            for i in range(3)
        ]

    def inject(first, last):
        for i in range(TILES):
            wait_tile(first + i)
        prepare(first, lhs_a, in_a, hot_a, 0)

        def pair(j, carry):
            one, two = first + (2 * j + 1) * TILES, first + (2 * j + 2) * TILES
            for i in range(2 * TILES):
                wait_tile(one + i)
            here = pl.multiple_of(j * width, width)
            then = pl.multiple_of((j + 1) * width, width)
            prepare(one, lhs_b, in_b, hot_b, here)
            gather_ring(lhs_a, hot_a, here)
            prepare(two, lhs_a, in_a, hot_a, then)
            gather_ring(lhs_b, hot_b, here)
            return carry

        half = chunks // 2
        lax.fori_loop(0, half - 1, pair, 0)
        end = first + (chunks - 1) * TILES
        for i in range(TILES - 1 if last else TILES):
            wait_tile(end + i)
        prepare(end, lhs_b, in_b, hot_b, (half - 1) * width)
        gather_ring(lhs_a, hot_a, (half - 1) * width)
        gather_ring(lhs_b, hot_b, (half - 1) * width)

    if n > span:
        def early(b, carry):
            inject(b * span + 1, False)
            for cell in range(cells):
                for i, f in enumerate(gather_core(cell)):
                    acc[cell, i * PAD + RING : (i + 1) * PAD, :] = f
            return carry

        lax.fori_loop(0, n // span - 1, early, 0)
    inject(n - span + 1, True)

    def stitch(low, high):
        lane = lax.broadcasted_iota(jnp.int32, low.shape, 1)
        up = jnp.where(lane < depth - 1, pltpu.roll(low, depth - 1, 1), 0.0)
        down = jnp.where(lane > 0, pltpu.roll(high, 1, 1), 0.0)
        return low + down, high + up

    def join(a, ra, b, rb, size):
        total = acc[a, ra : ra + size, :] + acc[b, rb : rb + size, :]
        acc[a, ra : ra + size, :] = total
        acc[b, rb : rb + size, :] = total

    def there(m):
        return neighbour(m, gx, gy, nx, ny)

    quad = 4 * halves
    line = (4 * cx - 1) * quad
    last = slice(depth - 128, depth)

    def strip_copy(src, dst, m, slot, where):
        dx, dy = MOVES[m]
        side, other = m % 2, 1 - m % 2
        return pltpu.make_async_remote_copy(
            src_ref=src.at[(side,) + where],
            dst_ref=dst.at[(other,) + where],
            send_sem=halo_send.at[slot, m],
            recv_sem=halo_recv.at[slot, m],
            device_id=(gx + dx, gy + dy),
            device_id_type=MESH,
        )

    def arriving(src, dst, m, slot, where):
        dx, dy = MOVES[m]
        return pltpu.make_async_remote_copy(
            src_ref=src.at[(m % 2,) + where],
            dst_ref=dst.at[(m % 2,) + where],
            send_sem=halo_send.at[slot, m],
            recv_sem=halo_recv.at[slot, m + 1 - 2 * (m % 2)],
            device_id=(gx + dx, gy + dy),
            device_id_type=MESH,
        )

    def part(c):
        return (pl.ds(c * line, line + (quad if c == 2 else 0)),)

    def pack_tips(rows):
        lane = lax.broadcasted_iota(jnp.int32, rows[0].shape, 1)
        total = rows[0]
        for c in (1, 2):
            total = jnp.where(lane == 127 - c, pltpu.roll(rows[c], 128 - c, 1), total)
        return total

    for c in range(3):
        o = c * PAD
        for cell in range(cells):
            low, high = stitch(acc[cell, o : o + 16, :], acc[cell, o + 64 : o + 80, :])
            acc[cell, o : o + 16, :] = low
            acc[cell, o + 64 : o + 80, :] = high
        for r in range(5):
            k = o + r * 16
            for y in range(cy):
                for x in range(cx - 1):
                    join(x * cy + y, k + 8, (x + 1) * cy + y, k, 5)
            for x in range(cx):
                for y in range(cy - 1):
                    a, b = x * cy + y, x * cy + y + 1
                    join(a, k + 13, b, k + 5, 3)
                    join(a, k + 4, b, k, 1)
                    join(a, k + 12, b, k + 8, 1)
        for side in (0, 1):
            low, mid, high = ((0, 5, 8), (4, 13, 12))[side]
            for x in range(cx):
                cell = x * cy + side * (cy - 1)
                for r in range(4):
                    k = o + r * 16
                    for h in range(halves):
                        lanes = slice(h * 128, (h + 1) * 128)
                        to = r * halves + h
                        at = c * line + x * 4 * quad + to
                        ys[side, pl.ds(at, 3, stride=quad), :] = acc[
                            cell, k + mid : k + mid + 3, lanes
                        ]
                        if x < cx - 1:
                            ys[side, at + 3 * quad : at + 3 * quad + 1, :] = acc[
                                cell, k + high : k + high + 1, lanes
                            ]
                        for e, row in ((0, low), (1, high)):
                            if x == e * (cx - 1):
                                at_e = (c * 2 + e) * quad + to
                                es[side, at_e : at_e + 1, :] = acc[
                                    cell, k + row : k + row + 1, lanes
                                ]
                k = o + 64
                tips[side, c, x * 4 : x * 4 + 3, :] = acc[cell, k + mid : k + mid + 3, last]
                for e, row in ((0, low), (1, high)):
                    if x == e * (cx - 1):
                        tips[2 + side, c, e : e + 1, :] = acc[cell, k + row : k + row + 1, last]
                if x < cx - 1:
                    tips[side, c, x * 4 + 3 : x * 4 + 4, :] = acc[cell, k + high : k + high + 1, last]
            if c == 2:
                ys[side, 3 * line : 3 * line + quad, :] = pack_tips([tips[side, d] for d in range(3)])
        for m in (2, 3):
            @pl.when(there(m))
            def _():
                strip_copy(ys, ry, m, c, part(c)).start()
        for y in range(cy):
            for side in (0, 1):
                cell = side * (cx - 1) * cy + y
                for h in range(halves):
                    for r in range(5):
                        k = o + r * 16 + side * 8
                        xs[side, c, pl.ds(r * rows_node + h * cy + y, 5, stride=5 * rows_node), :] = (
                            acc[cell, k : k + 5, h * 128 : (h + 1) * 128]
                        )
        for m in (0, 1):
            @pl.when(there(m))
            def _():
                strip_copy(xs, rx, m, c, (c,)).start()

    def place_rows(cell, c, values, row, size, node, step):
        start = ((cell // cy) * 3 + c) * 125 * rows_node + cell % cy
        for h in range(halves):
            at = start + h * cy + node * rows_node
            part = values[row : row + size, h * 128 : (h + 1) * 128]
            pre_h[pl.ds(at, size, stride=step * rows_node), :] = part

    for x in range(cx):
        for y in range(cy):
            cell = x * cy + y
            inner = gather_core(cell)
            for c in range(3):
                f = inner[c]
                low, high = stitch(f[0:8], f[32:40])
                lane = lax.broadcasted_iota(jnp.int32, (8, depth), 1)
                row = lax.broadcasted_iota(jnp.int32, (8, depth), 0)
                tail = f[40:48]
                up = pltpu.roll(pltpu.roll(tail, depth - 1, 1), 4, 0)
                down = pltpu.roll(pltpu.roll(tail, 1, 1), 4, 0)
                tail = (
                    tail
                    + jnp.where((row == 4) & (lane < depth - 1), up, 0.0)
                    + jnp.where((row == 0) & (lane > 0), down, 0.0)
                )
                planes = [low, f[8:16], f[16:24], f[24:32], high]
                for r in range(5):
                    ring = acc[cell, c * PAD + r * 16 : c * PAD + r * 16 + 16, :]
                    place_rows(cell, c, ring, 0, 5, r, 5)
                    place_rows(cell, c, ring, 5, 3, 25 + r, 25)
                    place_rows(cell, c, ring, 8, 5, 100 + r, 5)
                    place_rows(cell, c, ring, 13, 3, 45 + r, 25)
                    place_rows(cell, c, planes[r], 0, 3, 30 + r, 5)
                    place_rows(cell, c, planes[r], 3, 3, 55 + r, 5)
                    place_rows(cell, c, planes[r], 6, 2, 80 + r, 5)
                place_rows(cell, c, tail, 0, 5, 90, 1)

    for m in (0, 1):
        @pl.when(there(m))
        def _():
            for c in range(3):
                arriving(xs, rx, m, c, (c,)).wait_recv()
            for c in range(3):
                for side in (0, 1):
                    at = side * (20 * rows_node + cy - 1)
                    k = (c * 2 + m) * quad
                    es[side, k : k + quad, :] += rx[m, c, pl.ds(at, quad, stride=cy), :]
                    tip = at + 4 * rows_node + (halves - 1) * cy
                    tips[2 + side, c, m : m + 1, :] += rx[m, c, tip : tip + 1, :]

    for side in (0, 1):
        es[side, 6 * quad : 7 * quad, :] = pack_tips([tips[2 + side, d] for d in range(3)])
        m = 2 + side

        @pl.when(there(m))
        def _():
            strip_copy(es, re, m, 3, ()).start()

    def drain(k, c):
        tile_copy(k, lax.rem(me + k, n), me).wait_send()
        return c

    lax.fori_loop(1, n, drain, 0)
    for m in (0, 1):
        @pl.when(there(m))
        def _():
            for c in range(3):
                strip_copy(xs, rx, m, c, (c,)).wait_send()

    for m in (2, 3):
        @pl.when(there(m))
        def _():
            for c in range(3):
                arriving(ys, ry, m, c, part(c)).wait_recv()
                strip_copy(ys, ry, m, c, part(c)).wait_send()
            arriving(es, re, m, 3, ()).wait_recv()
            strip_copy(es, re, m, 3, ()).wait_send()


def finish_kernel(cx, cy, pre, rx, ry, re, out_h, buf, out_sem):
    total = buf.shape[0]
    block = total // (cx * 3)
    rows_node = block // 125
    halves = rows_node // cy
    plane, quad = 25 * rows_node, 4 * halves
    line = (4 * cx - 1) * quad
    lane = lax.broadcasted_iota(jnp.int32, (quad, 128), 1)
    row = lax.broadcasted_iota(jnp.int32, (quad, 128), 0)
    copies, done = [], 0
    for k in range(cx * 3):
        x, c = k // 3, k % 3
        base = k * block
        buf[base : base + block, :] = pre[base : base + block, :]
        if x == 0:
            buf[base : base + plane, :] += rx[0, c]
        if x == cx - 1:
            buf[base + 4 * plane : base + 5 * plane, :] += rx[1, c]
        for side in (0, 1):
            tips = pltpu.roll(ry[side, 3 * line : 3 * line + quad, :], c, 1)
            ends = pltpu.roll(re[side, 6 * quad : 7 * quad, :], c, 1)
            for p in range(5):
                pp = x * 4 + p
                if pp % (4 * cx) == 0:
                    e = pp // (4 * cx)
                    at = (c * 2 + e) * quad
                    values, tip = re[side, at : at + quad, :], ends[e : e + 1]
                else:
                    at = c * line + (pp - 1) * quad
                    values, tip = ry[side, at : at + quad, :], tips[pp - 1 : pp]
                ahead = pltpu.roll(values, 127, 1)
                beyond = jnp.where(row == halves - 1, tip, pltpu.roll(ahead, quad - 1, 0))
                upper = jnp.where(lane < 127, ahead, beyond)
                to = base + (p * 25 + side * 20) * rows_node + side * (cy - 1)
                buf[pl.ds(to, quad, stride=cy), :] += values
                buf[pl.ds(to + quad * cy, halves, stride=cy), :] += upper[:halves]
        upto = (k + 1) * block // 8 * 8
        copy = pltpu.make_async_copy(
            buf.at[pl.ds(done, upto - done)], out_h.at[pl.ds(done, upto - done)], out_sem.at[k]
        )
        copy.start()
        copies.append(copy)
        done = upto
    for copy in copies:
        copy.wait()


def anywhere(count):
    return [pl.BlockSpec(memory_space=pl.ANY)] * count


def body(nx, ny, wavefield, moduli, residuals, coords, angles, element_ids, counts):
    cx, cy, depth = wavefield.shape[0], wavefield.shape[1], wavefield.shape[4]
    n, slots = nx * ny, residuals.shape[2]
    cells, halves = cx * cy, depth // 128
    span = min(n, SPAN)
    width = TILES * slots
    rows = wavefield.transpose(0, 2, 3, 1, 4).reshape(cx, 3, 125, cy, halves, 128)
    rows = rows.transpose(0, 1, 2, 4, 3, 5).reshape(-1, 128)
    coords = coords.transpose(0, 2, 1, 3)
    moduli = moduli.reshape(cells, 2, depth)
    operands = [residuals, coords, angles, element_ids, counts, rows, moduli, *tables()]
    quad = 4 * halves
    received = [
        (2, 3, 25 * halves * cy, 128),
        (2, 3 * (4 * cx - 1) * quad + quad, 128),
        (2, 7 * quad, 128),
    ]
    scratch = [pltpu.VMEM(a.shape, a.dtype) for a in operands]
    scratch += [
        pltpu.VMEM((n, 8, slots), F32),
        pltpu.VMEM((n, 8, slots), F32),
        pltpu.VMEM((cells, 3 * PAD, depth), F32),
        pltpu.VMEM((6 * RING, width), BF16),
        pltpu.VMEM((6 * RING, width), BF16),
        pltpu.VMEM((6 * CORE, span * slots // 2), BF16),
        pltpu.VMEM((6 * CORE, span * slots // 2), BF16),
        pltpu.VMEM((span * slots // 2, cells * depth), BF16),
        pltpu.VMEM((span * slots // 2, cells * depth), BF16),
        pltpu.VMEM((2, 3, PAD, depth), F32),
    ]
    scratch += [pltpu.VMEM(s, F32) for s in received + [(4, 3, quad, 128)]]
    scratch += [
        pltpu.SemaphoreType.DMA((len(operands),)),
        pltpu.SemaphoreType.DMA((n,)),
        pltpu.SemaphoreType.DMA((n,)),
        pltpu.SemaphoreType.DMA((4, 4)),
        pltpu.SemaphoreType.DMA((4, 4)),
    ]
    parts = pl.pallas_call(
        functools.partial(step_kernel, nx, ny, cx, cy),
        out_shape=[pltpu.VMEM(s, F32) for s in [rows.shape] + received],
        in_specs=anywhere(len(operands)),
        out_specs=[pl.BlockSpec(memory_space=pltpu.VMEM)] * 4,
        scratch_shapes=scratch,
        compiler_params=pltpu.CompilerParams(collective_id=0, has_side_effects=True, vmem_limit_bytes=48 << 20),
    )(*[pltpu.with_memory_space_constraint(a, pltpu.HBM) for a in operands])
    force = pl.pallas_call(
        functools.partial(finish_kernel, cx, cy),
        out_shape=jax.ShapeDtypeStruct(rows.shape, F32),
        in_specs=[pl.BlockSpec(memory_space=pltpu.VMEM)] * 4,
        out_specs=anywhere(1)[0],
        scratch_shapes=[pltpu.VMEM(rows.shape, F32), pltpu.SemaphoreType.DMA((cx * 3,))],
        compiler_params=pltpu.CompilerParams(vmem_limit_bytes=16 << 20),
    )(*parts)
    force = force.reshape(cx, 3, 125, halves, cy, 128).transpose(0, 1, 2, 4, 3, 5)
    return force.reshape(cx, 3, 125, cy, depth).transpose(0, 3, 1, 2, 4)


def solution(mesh):
    in_specs = (
        P("gx", "gy", None, None, None),
        P("gx", "gy", None, None),
        P(("gx", "gy"), None, None),
        P(("gx", "gy"), None, None, None),
        P(("gx", "gy"), None, None, None),
        P(("gx", "gy"), None, None),
        P(("gx", "gy"), None),
    )
    out_specs = P("gx", "gy", None, None, None)
    return jax.shard_map(
        functools.partial(body, mesh.shape["gx"], mesh.shape["gy"]),
        mesh=mesh,
        in_specs=in_specs,
        out_specs=out_specs,
        check_vma=False,
    )
```

```python
import functools
import math

import jax
import jax.numpy as jnp
import numpy as np
from jax import lax
from jax.experimental import pallas as pl
from jax.experimental.pallas import tpu as pltpu
from jax.sharding import PartitionSpec as P

MESH = pl.DeviceIdType.MESH
F32, BF16 = jnp.float32, jnp.bfloat16
PAD = 128
SPAN = 32
TILES = 4
RING, CORE = 80, 48

EDGE = [(0, 0), (0, 1), (0, 2), (0, 3), (0, 4), (1, 0), (2, 0), (3, 0)]
EDGE += [(4, 0), (4, 1), (4, 2), (4, 3), (4, 4), (1, 4), (2, 4), (3, 4)]
INNER = [(1, 1), (1, 2), (1, 3), (2, 1), (2, 2), (2, 3), (3, 1), (3, 2)]
LAST = (3, 3)


def node_order():
    order = []
    for r in range(5):
        order += [(p * 5 + q) * 5 + r for p, q in EDGE]
    for r in range(5):
        order += [(p * 5 + q) * 5 + r for p, q in INNER]
    order += [(LAST[0] * 5 + LAST[1]) * 5 + r for r in range(5)]
    return np.array(order)


def gll_points():
    return np.array([-1.0, -math.sqrt(3.0 / 7.0), 0.0, math.sqrt(3.0 / 7.0), 1.0])


def gll_weights():
    return np.array([0.1, 49.0 / 90.0, 32.0 / 45.0, 49.0 / 90.0, 0.1])


def derivative_table():
    points = gll_points()
    table = np.zeros((5, 5))
    for row in range(5):
        for col in range(5):
            if row == col:
                table[row, col] = sum(
                    (1.0 / (points[col] - points[other]) for other in range(5) if other != col)
                )
            else:
                value = 1.0 / (points[col] - points[row])
                for other in range(5):
                    if other != col and other != row:
                        value = (
                            value * (points[row] - points[other]) / (points[col] - points[other])
                        )
                table[row, col] = value
    return table


def split_table(table):
    high = table.astype(BF16)
    return high, (table - high.astype(np.float64)).astype(BF16)


def roots(k):
    points = gll_points()
    others = [m for m in range(5) if m != k]
    return [points[m] for m in others], 1.0 / np.prod([points[k] - points[m] for m in others])


def tables():
    dm, eye = derivative_table(), np.eye(5)
    w1 = gll_weights()
    weight = (w1[:, None, None] * w1[None, :, None] * w1[None, None, :]).reshape(-1)
    dirs = [
        np.kron(np.kron(dm, eye), eye),
        np.kron(np.kron(eye, dm), eye),
        np.kron(np.kron(eye, eye), dm),
    ]
    order = node_order()
    grad = np.zeros((3 * PAD, PAD))
    back = np.zeros((PAD, 3 * PAD))
    for j in range(3):
        grad[j * PAD : j * PAD + 125, :125] = dirs[j][order]
        full = -dirs[j].T * weight[None, :]
        back[:125, j * PAD : j * PAD + 125] = full[order][:, order]
    gh, gl = split_table(grad)
    bh, bl = split_table(back)
    g1 = np.concatenate([gh, gh], 1)
    bs = np.concatenate([bh, bl], 0)
    consts = np.zeros((41, 8, 128), np.float32)
    for g, group in enumerate((EDGE[:8], EDGE[8:], INNER, [LAST] * 8)):
        for row, (p, q) in enumerate(group):
            rp, sp = roots(p)
            rq, sq = roots(q)
            for j in range(4):
                consts[g * 9 + j, row] = rp[j]
                consts[g * 9 + 4 + j, row] = rq[j]
            consts[g * 9 + 8, row] = sp * sq
    for r in range(5):
        rr, sr = roots(r)
        for j in range(4):
            consts[36 + j, r] = rr[j]
        consts[40, r] = sr
    return jnp.asarray(g1), jnp.asarray(gl), jnp.asarray(bs), jnp.asarray(consts)


def split(x):
    high = x.astype(BF16)
    return high, (x - high.astype(F32)).astype(BF16)


def dot(a, b):
    return jnp.dot(a, b, preferred_element_type=F32)


def sin_cos(x):
    h = x * 0.5
    h2 = h * h
    s = c = None
    for k in range(6, -1, -1):
        a = (-1.0) ** k / math.factorial(2 * k + 1)
        b = (-1.0) ** k / math.factorial(2 * k)
        s = jnp.full(x.shape, a, F32) if s is None else s * h2 + a
        c = jnp.full(x.shape, b, F32) if c is None else c * h2 + b
    s = s * h
    return 2.0 * s * c, 1.0 - 2.0 * s * s


def quartic(x, rows):
    a, b, c, d = [x - row for row in rows]
    ab, cd = a * b, c * d
    return ab * cd, (a + b) * cd + ab * (c + d)


MOVES = [(-1, 0), (1, 0), (0, -1), (0, 1)]


def neighbour(m, gx, gy, nx, ny):
    step = MOVES[m][m // 2]
    pos, total = ((gx, nx), (gy, ny))[m // 2]
    return pos > 0 if step < 0 else pos < total - 1


def step_kernel(
    nx, ny, cx, cy, resid_h, coord_h, angle_h, ids_h, count_h, u_h, mod_h, g1_h, g2_h, bs_h,
    consts_h, pre_h, rx, ry, re,
    resid, coord, angle, ids, count, u_ref, mod_ref, g1, g2, bs, consts,
    packed, got, acc, lhs_a, lhs_b, in_a, in_b, hot_a, hot_b, pad, xs, ys, es, tips,
    load_sem, send_sem, recv_sem, halo_send, halo_recv,
):
    n = nx * ny
    gx, gy = lax.axis_index("gx"), lax.axis_index("gy")
    me = gx * ny + gy
    cells, depth, slots = cx * cy, acc.shape[2], resid.shape[2]
    halves = depth // 128
    rows_node = halves * cy
    span = min(n, SPAN)
    chunks = span // TILES
    width = TILES * slots
    barrier = pltpu.get_barrier_semaphore()

    def after(k):
        to = me + k
        to = jnp.where(to >= n, to - n, to)
        return to, (lax.div(to, ny), lax.rem(to, ny))

    def greet(k):
        pl.semaphore_signal(barrier, inc=1, device_id=after(k)[1], device_id_type=MESH)

    def repeat(action):
        if n <= SPAN:
            for k in range(1, n):
                action(k)
        else:
            def one(k, c):
                action(k)
                return c

            lax.fori_loop(1, n, one, 0)

    pairs = [
        (count_h, count), (angle_h, angle), (resid_h, resid), (coord_h, coord), (ids_h, ids),
        (u_h, u_ref), (mod_h, mod_ref), (g1_h, g1), (g2_h, g2), (bs_h, bs), (consts_h, consts),
    ]
    loads = [pltpu.make_async_copy(a, b, load_sem.at[k]) for k, (a, b) in enumerate(pairs)]
    for copy in loads:
        copy.start()
    repeat(greet)
    for copy in loads[:5]:
        copy.wait()

    rows = lax.broadcasted_iota(jnp.int32, (n, n), 0)
    cols = lax.broadcasted_iota(jnp.int32, (n, n), 1)
    diagonal = jnp.where(rows == cols, count[...].astype(F32), 0.0)
    live_count = jnp.sum(diagonal, axis=1, keepdims=True)
    slot = lax.broadcasted_iota(jnp.int32, (n, slots), 1).astype(F32)
    sa, ca = sin_cos(angle[0, :, 0, :])
    sd, cd = sin_cos(angle[0, :, 1, :])
    packed[:, 0, :] = jnp.where(slot < live_count, resid[0], 0.0)
    for d in range(3):
        packed[:, 1 + d, :] = coord[0, d]
    packed[:, 4, :] = ca * cd
    packed[:, 5, :] = sa * cd
    packed[:, 6, :] = sd
    packed[:, 7, :] = ids[0].astype(F32)
    tips[...] = jnp.zeros_like(tips)
    for m in range(4):
        @pl.when(jnp.logical_not(neighbour(m, gx, gy, nx, ny)))
        def _():
            for hole in ((rx,), (ry, re))[m // 2]:
                hole[m % 2] = jnp.zeros(hole.shape[1:], F32)

    pad[...] = jnp.zeros_like(pad)
    for copy in loads[5:]:
        copy.wait()

    def stiff(cell, slab):
        g = []
        for c in range(3):
            start = ((cell // cy) * 3 + c) * 125 * rows_node + cell % cy
            for h in range(halves):
                pad[slab, c, 0:125, h * 128 : (h + 1) * 128] = u_ref[
                    pl.ds(start + h * cy, 125, stride=rows_node), :
                ]
            high, low = split(pad[slab, c])
            r = dot(g1[...], jnp.concatenate([high, low], axis=0)) + dot(g2[...], high)
            g.append([r[j * PAD : (j + 1) * PAD] for j in range(3)])
        lam, mu = mod_ref[cell, 0:1, :], mod_ref[cell, 1:2, :]
        press = lam * (g[0][0] + g[1][1] + g[2][2])
        for i in range(3):
            parts = []
            for j in range(3):
                s = mu * (g[i][j] + g[j][i])
                parts.append(s + press if i == j else s)
            high, low = split(jnp.concatenate(parts, axis=0))
            r = dot(bs[...], high)
            acc[cell, i * PAD : (i + 1) * PAD, :] = r[:PAD] + r[PAD:] + dot(bs[:PAD], low)

    early = 0
    for cell in range(early):
        stiff(cell, cell % 2)
    pl.semaphore_wait(barrier, n - 1)

    def tile_copy(k, at):
        to, where = after(k)
        return pltpu.make_async_remote_copy(
            src_ref=packed.at[to],
            dst_ref=got.at[at],
            send_sem=send_sem.at[0],
            recv_sem=recv_sem.at[(k - 1) // TILES],
            device_id=where,
            device_id_type=MESH,
        )

    def send(k):
        tile_copy(k, me).start()

    repeat(send)
    got[me] = packed[me]
    for cell in range(early, cells):
        stiff(cell, cell % 2)

    def many(count, group):
        other = lax.rem(me + 1, n)
        return pltpu.make_async_remote_copy(
            src_ref=packed.at[pl.ds(0, count)],
            dst_ref=got.at[pl.ds(0, count)],
            send_sem=send_sem.at[0],
            recv_sem=recv_sem.at[group],
            device_id=(other // ny, lax.rem(other, ny)),
            device_id_type=MESH,
        )

    def wait_tiles(first, count):
        many(count, (first - 1) // TILES).wait_recv()

    def prepare(first, ring, inner, hot, at):
        tiles = [got[lax.rem(me - (first + i) + n, n)] for i in range(TILES)]
        tile = jnp.concatenate(tiles, axis=1)

        def const(k):
            return jnp.concatenate([consts[k]] * TILES, axis=1)

        v = tile[0:1]
        t = [tile[4 + i : 5 + i] for i in range(3)]
        x, y, z = [jnp.broadcast_to(tile[1 + d : 2 + d], (8, width)) for d in range(3)]
        lz, dz = quartic(z, [const(36 + j) for j in range(4)])
        lz, dz = lz * const(40), dz * (const(40) * t[2])
        first_of, second_of = [], []
        for g in range(4):
            lx, dx = quartic(x, [const(g * 9 + j) for j in range(4)])
            ly, dy = quartic(y, [const(g * 9 + 4 + j) for j in range(4)])
            scale = const(g * 9 + 8)
            first_of.append(scale * ((t[0] * dx) * ly + (t[1] * dy) * lx))
            second_of.append(scale * (lx * ly))
        edge, core = [], []
        for r in range(5):
            a = jnp.broadcast_to(lz[r : r + 1], (8, width))
            b = jnp.broadcast_to(dz[r : r + 1], (8, width))
            edge += [first_of[g] * a + second_of[g] * b for g in (0, 1)]
            core.append(first_of[2] * a + second_of[2] * b)
        core.append(first_of[3] * lz + second_of[3] * dz)
        edge, core = jnp.concatenate(edge, axis=0), jnp.concatenate(core, axis=0)
        for i in range(3):
            w = v * t[i]
            high, low = split(edge * w)
            ring[2 * i * RING : (2 * i + 1) * RING, :] = high
            ring[(2 * i + 1) * RING : (2 * i + 2) * RING, :] = low
            high, low = split(core * w)
            inner[2 * i * CORE : (2 * i + 1) * CORE, pl.ds(at, width)] = high
            inner[(2 * i + 1) * CORE : (2 * i + 2) * CORE, pl.ds(at, width)] = low
        number = lax.broadcasted_iota(jnp.int32, (slots, cells * depth), 1).astype(F32)
        for i in range(TILES):
            ident = tiles[i].T[:, 7:8]
            hot[pl.ds(at + i * slots, slots), :] = jnp.where(number == ident, 1.0, 0.0).astype(BF16)

    def gather_ring(ring, hot, at):
        for cell in range(cells):
            r = dot(ring[...], hot[pl.ds(at, width), cell * depth : (cell + 1) * depth])
            for i in range(3):
                acc[cell, i * PAD : i * PAD + RING, :] += (
                    r[2 * i * RING : (2 * i + 1) * RING]
                    + r[(2 * i + 1) * RING : (2 * i + 2) * RING]
                )

    def gather_core(cell):
        where = slice(cell * depth, (cell + 1) * depth)
        r = dot(in_a[...], hot_a[:, where]) + dot(in_b[...], hot_b[:, where])
        return [
            acc[cell, i * PAD + RING : (i + 1) * PAD, :]
            + r[2 * i * CORE : (2 * i + 1) * CORE]
            + r[(2 * i + 1) * CORE : (2 * i + 2) * CORE]
            for i in range(3)
        ]

    def inject(first, last):
        wait_tiles(first, TILES)
        prepare(first, lhs_a, in_a, hot_a, 0)

        def pair(j, carry):
            one, two = first + (2 * j + 1) * TILES, first + (2 * j + 2) * TILES
            wait_tiles(one, TILES)
            here = pl.multiple_of(j * width, width)
            then = pl.multiple_of((j + 1) * width, width)
            prepare(one, lhs_b, in_b, hot_b, here)
            gather_ring(lhs_a, hot_a, here)
            wait_tiles(two, TILES)
            prepare(two, lhs_a, in_a, hot_a, then)
            gather_ring(lhs_b, hot_b, here)
            return carry

        half = chunks // 2
        lax.fori_loop(0, half - 1, pair, 0)
        end = first + (chunks - 1) * TILES
        wait_tiles(end, TILES - 1 if last else TILES)
        prepare(end, lhs_b, in_b, hot_b, (half - 1) * width)
        gather_ring(lhs_a, hot_a, (half - 1) * width)
        gather_ring(lhs_b, hot_b, (half - 1) * width)

    if n > span:
        def early(b, carry):
            inject(b * span + 1, False)
            for cell in range(cells):
                for i, f in enumerate(gather_core(cell)):
                    acc[cell, i * PAD + RING : (i + 1) * PAD, :] = f
            return carry

        lax.fori_loop(0, n // span - 1, early, 0)
    inject(n - span + 1, True)

    def stitch(low, high):
        lane = lax.broadcasted_iota(jnp.int32, low.shape, 1)
        up = jnp.where(lane < depth - 1, pltpu.roll(low, depth - 1, 1), 0.0)
        down = jnp.where(lane > 0, pltpu.roll(high, 1, 1), 0.0)
        return low + down, high + up

    def join(a, ra, b, rb, size):
        total = acc[a, ra : ra + size, :] + acc[b, rb : rb + size, :]
        acc[a, ra : ra + size, :] = total
        acc[b, rb : rb + size, :] = total

    def there(m):
        return neighbour(m, gx, gy, nx, ny)

    quad = 4 * halves
    line = (4 * cx - 1) * quad
    last = slice(depth - 128, depth)

    def strip_copy(src, dst, m, slot, where):
        dx, dy = MOVES[m]
        side, other = m % 2, 1 - m % 2
        return pltpu.make_async_remote_copy(
            src_ref=src.at[(side,) + where],
            dst_ref=dst.at[(other,) + where],
            send_sem=halo_send.at[2 * slot + m],
            recv_sem=halo_recv.at[2 * slot + m],
            device_id=(gx + dx, gy + dy),
            device_id_type=MESH,
        )

    def arriving(src, dst, m, slot, where):
        dx, dy = MOVES[m]
        return pltpu.make_async_remote_copy(
            src_ref=src.at[(m % 2,) + where],
            dst_ref=dst.at[(m % 2,) + where],
            send_sem=halo_send.at[2 * slot + m],
            recv_sem=halo_recv.at[2 * slot + m + 1 - 2 * (m % 2)],
            device_id=(gx + dx, gy + dy),
            device_id_type=MESH,
        )

    def part(c):
        return (pl.ds(c * line, line + (quad if c == 2 else 0)),)

    def pack_tips(rows):
        lane = lax.broadcasted_iota(jnp.int32, rows[0].shape, 1)
        total = rows[0]
        for c in (1, 2):
            total = jnp.where(lane == 127 - c, pltpu.roll(rows[c], 128 - c, 1), total)
        return total

    for c in range(3):
        o = c * PAD
        for cell in range(cells):
            low, high = stitch(acc[cell, o : o + 16, :], acc[cell, o + 64 : o + 80, :])
            acc[cell, o : o + 16, :] = low
            acc[cell, o + 64 : o + 80, :] = high
        for r in range(5):
            k = o + r * 16
            for y in range(cy):
                for x in range(cx - 1):
                    join(x * cy + y, k + 8, (x + 1) * cy + y, k, 5)
            for x in range(cx):
                for y in range(cy - 1):
                    a, b = x * cy + y, x * cy + y + 1
                    join(a, k + 13, b, k + 5, 3)
                    join(a, k + 4, b, k, 1)
                    join(a, k + 12, b, k + 8, 1)
        for y in range(cy):
            for side in (0, 1):
                cell = side * (cx - 1) * cy + y
                for h in range(halves):
                    for r in range(5):
                        k = o + r * 16 + side * 8
                        xs[side, c, pl.ds(r * rows_node + h * cy + y, 5, stride=5 * rows_node), :] = (
                            acc[cell, k : k + 5, h * 128 : (h + 1) * 128]
                        )
        for m in (0, 1):
            @pl.when(there(m))
            def _():
                strip_copy(xs, rx, m, 0, (c,)).start()
        for side in (0, 1):
            low, mid, high = ((0, 5, 8), (4, 13, 12))[side]
            for x in range(cx):
                cell = x * cy + side * (cy - 1)
                for r in range(4):
                    k = o + r * 16
                    for h in range(halves):
                        lanes = slice(h * 128, (h + 1) * 128)
                        to = r * halves + h
                        at = c * line + x * 4 * quad + to
                        ys[side, pl.ds(at, 3, stride=quad), :] = acc[
                            cell, k + mid : k + mid + 3, lanes
                        ]
                        if x < cx - 1:
                            ys[side, at + 3 * quad : at + 3 * quad + 1, :] = acc[
                                cell, k + high : k + high + 1, lanes
                            ]
                        for e, row in ((0, low), (1, high)):
                            if x == e * (cx - 1):
                                at_e = (c * 2 + e) * quad + to
                                es[side, at_e : at_e + 1, :] = acc[
                                    cell, k + row : k + row + 1, lanes
                                ]
                k = o + 64
                tips[side, c, x * 4 : x * 4 + 3, :] = acc[cell, k + mid : k + mid + 3, last]
                for e, row in ((0, low), (1, high)):
                    if x == e * (cx - 1):
                        tips[2 + side, c, e : e + 1, :] = acc[cell, k + row : k + row + 1, last]
                if x < cx - 1:
                    tips[side, c, x * 4 + 3 : x * 4 + 4, :] = acc[cell, k + high : k + high + 1, last]
            if c == 2:
                ys[side, 3 * line : 3 * line + quad, :] = pack_tips([tips[side, d] for d in range(3)])
        for m in (2, 3):
            @pl.when(there(m))
            def _():
                strip_copy(ys, ry, m, 0, part(c)).start()

    def place_rows(cell, c, values, row, size, node, step):
        start = ((cell // cy) * 3 + c) * 125 * rows_node + cell % cy
        for h in range(halves):
            at = start + h * cy + node * rows_node
            part = values[row : row + size, h * 128 : (h + 1) * 128]
            pre_h[pl.ds(at, size, stride=step * rows_node), :] = part

    for x in range(cx):
        for y in range(cy):
            cell = x * cy + y
            inner = gather_core(cell)
            for c in range(3):
                f = inner[c]
                low, high = stitch(f[0:8], f[32:40])
                lane = lax.broadcasted_iota(jnp.int32, (8, depth), 1)
                row = lax.broadcasted_iota(jnp.int32, (8, depth), 0)
                tail = f[40:48]
                up = pltpu.roll(pltpu.roll(tail, depth - 1, 1), 4, 0)
                down = pltpu.roll(pltpu.roll(tail, 1, 1), 4, 0)
                tail = (
                    tail
                    + jnp.where((row == 4) & (lane < depth - 1), up, 0.0)
                    + jnp.where((row == 0) & (lane > 0), down, 0.0)
                )
                planes = [low, f[8:16], f[16:24], f[24:32], high]
                for r in range(5):
                    ring = acc[cell, c * PAD + r * 16 : c * PAD + r * 16 + 16, :]
                    place_rows(cell, c, ring, 0, 5, r, 5)
                    place_rows(cell, c, ring, 5, 3, 25 + r, 25)
                    place_rows(cell, c, ring, 8, 5, 100 + r, 5)
                    place_rows(cell, c, ring, 13, 3, 45 + r, 25)
                    place_rows(cell, c, planes[r], 0, 3, 30 + r, 5)
                    place_rows(cell, c, planes[r], 3, 3, 55 + r, 5)
                    place_rows(cell, c, planes[r], 6, 2, 80 + r, 5)
                place_rows(cell, c, tail, 0, 5, 90, 1)

    for m in (0, 1):
        @pl.when(there(m))
        def _():
            arriving(xs, rx, m, 0, ()).wait_recv()
            for c in range(3):
                for side in (0, 1):
                    at = side * (20 * rows_node + cy - 1)
                    k = (c * 2 + m) * quad
                    es[side, k : k + quad, :] += rx[m, c, pl.ds(at, quad, stride=cy), :]
                    tip = at + 4 * rows_node + (halves - 1) * cy
                    tips[2 + side, c, m : m + 1, :] += rx[m, c, tip : tip + 1, :]

    for side in (0, 1):
        es[side, 6 * quad : 7 * quad, :] = pack_tips([tips[2 + side, d] for d in range(3)])
        m = 2 + side

        @pl.when(there(m))
        def _():
            strip_copy(es, re, m, 1, ()).start()

    many(n - 1, 0).wait_send()
    for m in (0, 1):
        @pl.when(there(m))
        def _():
            strip_copy(xs, rx, m, 0, ()).wait_send()

    for m in (2, 3):
        @pl.when(there(m))
        def _():
            arriving(ys, ry, m, 0, ()).wait_recv()
            strip_copy(ys, ry, m, 0, ()).wait_send()
            arriving(es, re, m, 1, ()).wait_recv()
            strip_copy(es, re, m, 1, ()).wait_send()


def finish_kernel(cx, cy, pre, rx, ry, re, out_h, buf, out_sem):
    total = buf.shape[0]
    block = total // (cx * 3)
    rows_node = block // 125
    halves = rows_node // cy
    plane, quad = 25 * rows_node, 4 * halves
    line = (4 * cx - 1) * quad
    lane = lax.broadcasted_iota(jnp.int32, (quad, 128), 1)
    row = lax.broadcasted_iota(jnp.int32, (quad, 128), 0)
    copies, done = [], 0
    for k in range(cx * 3):
        x, c = k // 3, k % 3
        base = k * block
        buf[base : base + block, :] = pre[base : base + block, :]
        if x == 0:
            buf[base : base + plane, :] += rx[0, c, :plane]
        if x == cx - 1:
            buf[base + 4 * plane : base + 5 * plane, :] += rx[1, c, :plane]
        for side in (0, 1):
            tips = pltpu.roll(ry[side, 3 * line : 3 * line + quad, :], c, 1)
            ends = pltpu.roll(re[side, 6 * quad : 7 * quad, :], c, 1)
            for p in range(5):
                pp = x * 4 + p
                if pp % (4 * cx) == 0:
                    e = pp // (4 * cx)
                    at = (c * 2 + e) * quad
                    values, tip = re[side, at : at + quad, :], ends[e : e + 1]
                else:
                    at = c * line + (pp - 1) * quad
                    values, tip = ry[side, at : at + quad, :], tips[pp - 1 : pp]
                ahead = pltpu.roll(values, 127, 1)
                beyond = jnp.where(row == halves - 1, tip, pltpu.roll(ahead, quad - 1, 0))
                upper = jnp.where(lane < 127, ahead, beyond)
                to = base + (p * 25 + side * 20) * rows_node + side * (cy - 1)
                buf[pl.ds(to, quad, stride=cy), :] += values
                buf[pl.ds(to + quad * cy, halves, stride=cy), :] += upper[:halves]
        upto = (k + 1) * block // 8 * 8
        copy = pltpu.make_async_copy(
            buf.at[pl.ds(done, upto - done)], out_h.at[pl.ds(done, upto - done)], out_sem.at[k]
        )
        copy.start()
        copies.append(copy)
        done = upto
    for copy in copies:
        copy.wait()


def anywhere(count):
    return [pl.BlockSpec(memory_space=pl.ANY)] * count


def body(nx, ny, wavefield, moduli, residuals, coords, angles, element_ids, counts):
    cx, cy, depth = wavefield.shape[0], wavefield.shape[1], wavefield.shape[4]
    n, slots = nx * ny, residuals.shape[2]
    cells, halves = cx * cy, depth // 128
    span = min(n, SPAN)
    width = TILES * slots
    rows = wavefield.transpose(0, 2, 3, 1, 4).reshape(cx, 3, 125, cy, halves, 128)
    rows = rows.transpose(0, 1, 2, 4, 3, 5).reshape(-1, 128)
    coords = coords.transpose(0, 2, 1, 3)
    moduli = moduli.reshape(cells, 2, depth)
    operands = [residuals, coords, angles, element_ids, counts, rows, moduli, *tables()]
    quad = 4 * halves
    received = [
        (2, 3, -(-25 * halves * cy // 8) * 8, 128),
        (2, 3 * (4 * cx - 1) * quad + quad, 128),
        (2, 7 * quad, 128),
    ]
    scratch = [pltpu.VMEM(a.shape, a.dtype) for a in operands]
    scratch += [
        pltpu.VMEM((n, 8, slots), F32),
        pltpu.VMEM((n, 8, slots), F32),
        pltpu.VMEM((cells, 3 * PAD, depth), F32),
        pltpu.VMEM((6 * RING, width), BF16),
        pltpu.VMEM((6 * RING, width), BF16),
        pltpu.VMEM((6 * CORE, span * slots // 2), BF16),
        pltpu.VMEM((6 * CORE, span * slots // 2), BF16),
        pltpu.VMEM((span * slots // 2, cells * depth), BF16),
        pltpu.VMEM((span * slots // 2, cells * depth), BF16),
        pltpu.VMEM((2, 3, PAD, depth), F32),
    ]
    scratch += [pltpu.VMEM(s, F32) for s in received + [(4, 3, quad, 128)]]
    scratch += [
        pltpu.SemaphoreType.DMA((len(operands),)),
        pltpu.SemaphoreType.DMA((1,)),
        pltpu.SemaphoreType.DMA((n // TILES,)),
        pltpu.SemaphoreType.DMA((6,)),
        pltpu.SemaphoreType.DMA((6,)),
    ]
    parts = pl.pallas_call(
        functools.partial(step_kernel, nx, ny, cx, cy),
        out_shape=[pltpu.VMEM(s, F32) for s in [rows.shape] + received],
        in_specs=anywhere(len(operands)),
        out_specs=[pl.BlockSpec(memory_space=pltpu.VMEM)] * 4,
        scratch_shapes=scratch,
        compiler_params=pltpu.CompilerParams(collective_id=0, has_side_effects=True, vmem_limit_bytes=48 << 20),
    )(*[pltpu.with_memory_space_constraint(a, pltpu.HBM) for a in operands])
    force = pl.pallas_call(
        functools.partial(finish_kernel, cx, cy),
        out_shape=jax.ShapeDtypeStruct(rows.shape, F32),
        in_specs=[pl.BlockSpec(memory_space=pltpu.VMEM)] * 4,
        out_specs=anywhere(1)[0],
        scratch_shapes=[pltpu.VMEM(rows.shape, F32), pltpu.SemaphoreType.DMA((cx * 3,))],
        compiler_params=pltpu.CompilerParams(vmem_limit_bytes=16 << 20),
    )(*parts)
    force = force.reshape(cx, 3, 125, halves, cy, 128).transpose(0, 1, 2, 4, 3, 5)
    return force.reshape(cx, 3, 125, cy, depth).transpose(0, 3, 1, 2, 4)


def solution(mesh):
    in_specs = (
        P("gx", "gy", None, None, None),
        P("gx", "gy", None, None),
        P(("gx", "gy"), None, None),
        P(("gx", "gy"), None, None, None),
        P(("gx", "gy"), None, None, None),
        P(("gx", "gy"), None, None),
        P(("gx", "gy"), None),
    )
    out_specs = P("gx", "gy", None, None, None)
    return jax.shard_map(
        functools.partial(body, mesh.shape["gx"], mesh.shape["gy"]),
        mesh=mesh,
        in_specs=in_specs,
        out_specs=out_specs,
        check_vma=False,
    )
```

```python
import functools
import math

import jax
import jax.numpy as jnp
import numpy as np
from jax import lax
from jax.experimental import pallas as pl
from jax.experimental.pallas import tpu as pltpu
from jax.sharding import PartitionSpec as P

MESH = pl.DeviceIdType.MESH
F32, BF16 = jnp.float32, jnp.bfloat16
PAD = 128
SPAN = 32
TILES = 4
RING, CORE = 80, 48

EDGE = [(0, 0), (0, 1), (0, 2), (0, 3), (0, 4), (1, 0), (2, 0), (3, 0)]
EDGE += [(4, 0), (4, 1), (4, 2), (4, 3), (4, 4), (1, 4), (2, 4), (3, 4)]
INNER = [(1, 1), (1, 2), (1, 3), (2, 1), (2, 2), (2, 3), (3, 1), (3, 2)]
LAST = (3, 3)


def node_order():
    order = []
    for r in range(5):
        order += [(p * 5 + q) * 5 + r for p, q in EDGE]
    for r in range(5):
        order += [(p * 5 + q) * 5 + r for p, q in INNER]
    order += [(LAST[0] * 5 + LAST[1]) * 5 + r for r in range(5)]
    return np.array(order)


def gll_points():
    return np.array([-1.0, -math.sqrt(3.0 / 7.0), 0.0, math.sqrt(3.0 / 7.0), 1.0])


def gll_weights():
    return np.array([0.1, 49.0 / 90.0, 32.0 / 45.0, 49.0 / 90.0, 0.1])


def derivative_table():
    points = gll_points()
    table = np.zeros((5, 5))
    for row in range(5):
        for col in range(5):
            if row == col:
                table[row, col] = sum(
                    (1.0 / (points[col] - points[other]) for other in range(5) if other != col)
                )
            else:
                value = 1.0 / (points[col] - points[row])
                for other in range(5):
                    if other != col and other != row:
                        value = (
                            value * (points[row] - points[other]) / (points[col] - points[other])
                        )
                table[row, col] = value
    return table


def split_table(table):
    high = table.astype(BF16)
    return high, (table - high.astype(np.float64)).astype(BF16)


def roots(k):
    points = gll_points()
    others = [m for m in range(5) if m != k]
    return [points[m] for m in others], 1.0 / np.prod([points[k] - points[m] for m in others])


def tables():
    dm, eye = derivative_table(), np.eye(5)
    w1 = gll_weights()
    weight = (w1[:, None, None] * w1[None, :, None] * w1[None, None, :]).reshape(-1)
    dirs = [
        np.kron(np.kron(dm, eye), eye),
        np.kron(np.kron(eye, dm), eye),
        np.kron(np.kron(eye, eye), dm),
    ]
    order = node_order()
    grad = np.zeros((3 * PAD, PAD))
    back = np.zeros((PAD, 3 * PAD))
    for j in range(3):
        grad[j * PAD : j * PAD + 125, :125] = dirs[j][order]
        full = -dirs[j].T * weight[None, :]
        back[:125, j * PAD : j * PAD + 125] = full[order][:, order]
    gh, gl = split_table(grad)
    bh, bl = split_table(back)
    g1 = np.concatenate([gh, gh], 1)
    bs = np.concatenate([bh, bl], 0)
    consts = np.zeros((41, 8, 128), np.float32)
    for g, group in enumerate((EDGE[:8], EDGE[8:], INNER, [LAST] * 8)):
        for row, (p, q) in enumerate(group):
            rp, sp = roots(p)
            rq, sq = roots(q)
            for j in range(4):
                consts[g * 9 + j, row] = rp[j]
                consts[g * 9 + 4 + j, row] = rq[j]
            consts[g * 9 + 8, row] = sp * sq
    for r in range(5):
        rr, sr = roots(r)
        for j in range(4):
            consts[36 + j, r] = rr[j]
        consts[40, r] = sr
    return jnp.asarray(g1), jnp.asarray(gl), jnp.asarray(bs), jnp.asarray(consts)


def split(x):
    high = x.astype(BF16)
    return high, (x - high.astype(F32)).astype(BF16)


def dot(a, b):
    return jnp.dot(a, b, preferred_element_type=F32)


def sin_cos(x):
    h = x * 0.5
    h2 = h * h
    s = c = None
    for k in range(6, -1, -1):
        a = (-1.0) ** k / math.factorial(2 * k + 1)
        b = (-1.0) ** k / math.factorial(2 * k)
        s = jnp.full(x.shape, a, F32) if s is None else s * h2 + a
        c = jnp.full(x.shape, b, F32) if c is None else c * h2 + b
    s = s * h
    return 2.0 * s * c, 1.0 - 2.0 * s * s


def quartic(x, rows):
    a, b, c, d = [x - row for row in rows]
    ab, cd = a * b, c * d
    return ab * cd, (a + b) * cd + ab * (c + d)


MOVES = [(-1, 0), (1, 0), (0, -1), (0, 1)]


def neighbour(m, gx, gy, nx, ny):
    step = MOVES[m][m // 2]
    pos, total = ((gx, nx), (gy, ny))[m // 2]
    return pos > 0 if step < 0 else pos < total - 1


def step_kernel(
    nx, ny, cx, cy, resid_h, coord_h, angle_h, ids_h, count_h, u_h, mod_h, g1_h, g2_h, bs_h,
    consts_h, pre_h, rx, ry, re,
    resid, coord, angle, ids, count, u_ref, mod_ref, g1, g2, bs, consts,
    packed, got, acc, lhs_a, lhs_b, in_a, in_b, hot_a, hot_b, pad, xs, ys, es, tips,
    load_sem, send_sem, recv_sem, halo_send, halo_recv,
):
    n = nx * ny
    gx, gy = lax.axis_index("gx"), lax.axis_index("gy")
    me = gx * ny + gy
    cells, depth, slots = cx * cy, acc.shape[2], resid.shape[2]
    halves = depth // 128
    rows_node = halves * cy
    span = min(n, SPAN)
    chunks = span // TILES
    width = TILES * slots
    barrier = pltpu.get_barrier_semaphore()

    def after(k):
        to = me + k
        to = jnp.where(to >= n, to - n, to)
        return to, (lax.div(to, ny), lax.rem(to, ny))

    def greet(k):
        pl.semaphore_signal(barrier, inc=1, device_id=after(k)[1], device_id_type=MESH)

    def repeat(action):
        if n <= SPAN:
            for k in range(1, n):
                action(k)
        else:
            def one(k, c):
                action(k)
                return c

            lax.fori_loop(1, n, one, 0)

    pairs = [
        (count_h, count), (angle_h, angle), (resid_h, resid), (coord_h, coord), (ids_h, ids),
        (u_h, u_ref), (mod_h, mod_ref), (g1_h, g1), (g2_h, g2), (bs_h, bs), (consts_h, consts),
    ]
    loads = [pltpu.make_async_copy(a, b, load_sem.at[k]) for k, (a, b) in enumerate(pairs)]
    for copy in loads:
        copy.start()
    repeat(greet)
    for copy in loads[:5]:
        copy.wait()

    rows = lax.broadcasted_iota(jnp.int32, (n, n), 0)
    cols = lax.broadcasted_iota(jnp.int32, (n, n), 1)
    diagonal = jnp.where(rows == cols, count[...].astype(F32), 0.0)
    live_count = jnp.sum(diagonal, axis=1, keepdims=True)
    slot = lax.broadcasted_iota(jnp.int32, (n, slots), 1).astype(F32)
    sa, ca = sin_cos(angle[0, :, 0, :])
    sd, cd = sin_cos(angle[0, :, 1, :])
    packed[:, 0, :] = jnp.where(slot < live_count, resid[0], 0.0)
    for d in range(3):
        packed[:, 1 + d, :] = coord[0, d]
    packed[:, 4, :] = ca * cd
    packed[:, 5, :] = sa * cd
    packed[:, 6, :] = sd
    packed[:, 7, :] = ids[0].astype(F32)
    tips[...] = jnp.zeros_like(tips)
    for m in range(4):
        @pl.when(jnp.logical_not(neighbour(m, gx, gy, nx, ny)))
        def _():
            for hole in ((rx,), (ry, re))[m // 2]:
                hole[m % 2] = jnp.zeros(hole.shape[1:], F32)

    pad[...] = jnp.zeros_like(pad)
    for copy in loads[5:]:
        copy.wait()

    def strain(cell, slab, c):
        start = ((cell // cy) * 3 + c) * 125 * rows_node + cell % cy
        for h in range(halves):
            pad[slab, c, 0:125, h * 128 : (h + 1) * 128] = u_ref[
                pl.ds(start + h * cy, 125, stride=rows_node), :
            ]
        high, low = split(pad[slab, c])
        r = dot(g1[...], jnp.concatenate([high, low], axis=0)) + dot(g2[...], high)
        return [r[j * PAD : (j + 1) * PAD] for j in range(3)]

    def stiff(group):
        g = {cell: [] for cell in group}
        for c in range(3):
            for cell in group:
                g[cell].append(strain(cell, cell % len(group), c))
        press = {}
        for cell in group:
            press[cell] = mod_ref[cell, 0:1, :] * (g[cell][0][0] + g[cell][1][1] + g[cell][2][2])
        for i in range(3):
            for cell in group:
                mu, parts = mod_ref[cell, 1:2, :], []
                for j in range(3):
                    s = mu * (g[cell][i][j] + g[cell][j][i])
                    parts.append(s + press[cell] if i == j else s)
                high, low = split(jnp.concatenate(parts, axis=0))
                r = dot(bs[...], high)
                acc[cell, i * PAD : (i + 1) * PAD, :] = r[:PAD] + r[PAD:] + dot(bs[:PAD], low)

    pl.semaphore_wait(barrier, n - 1)

    def tile_copy(k, at):
        to, where = after(k)
        return pltpu.make_async_remote_copy(
            src_ref=packed.at[to],
            dst_ref=got.at[at],
            send_sem=send_sem.at[0],
            recv_sem=recv_sem.at[(k - 1) // TILES],
            device_id=where,
            device_id_type=MESH,
        )

    def send(k):
        tile_copy(k, me).start()

    repeat(send)
    got[me] = packed[me]
    for first_cell in range(0, cells, 2):
        stiff(range(first_cell, min(first_cell + 2, cells)))

    def many(count, group):
        other = lax.rem(me + 1, n)
        return pltpu.make_async_remote_copy(
            src_ref=packed.at[pl.ds(0, count)],
            dst_ref=got.at[pl.ds(0, count)],
            send_sem=send_sem.at[0],
            recv_sem=recv_sem.at[group],
            device_id=(other // ny, lax.rem(other, ny)),
            device_id_type=MESH,
        )

    def wait_tiles(first, count):
        many(count, (first - 1) // TILES).wait_recv()

    def prepare(first, ring, inner, hot, at):
        tiles = [got[lax.rem(me - (first + i) + n, n)] for i in range(TILES)]
        tile = jnp.concatenate(tiles, axis=1)

        def const(k):
            return jnp.concatenate([consts[k]] * TILES, axis=1)

        v = tile[0:1]
        t = [tile[4 + i : 5 + i] for i in range(3)]
        x, y, z = [jnp.broadcast_to(tile[1 + d : 2 + d], (8, width)) for d in range(3)]
        lz, dz = quartic(z, [const(36 + j) for j in range(4)])
        lz, dz = lz * const(40), dz * (const(40) * t[2])
        first_of, second_of = [], []
        for g in range(4):
            lx, dx = quartic(x, [const(g * 9 + j) for j in range(4)])
            ly, dy = quartic(y, [const(g * 9 + 4 + j) for j in range(4)])
            scale = const(g * 9 + 8)
            first_of.append(scale * ((t[0] * dx) * ly + (t[1] * dy) * lx))
            second_of.append(scale * (lx * ly))
        edge, core = [], []
        for r in range(5):
            a = jnp.broadcast_to(lz[r : r + 1], (8, width))
            b = jnp.broadcast_to(dz[r : r + 1], (8, width))
            edge += [first_of[g] * a + second_of[g] * b for g in (0, 1)]
            core.append(first_of[2] * a + second_of[2] * b)
        core.append(first_of[3] * lz + second_of[3] * dz)
        edge, core = jnp.concatenate(edge, axis=0), jnp.concatenate(core, axis=0)
        for i in range(3):
            w = v * t[i]
            high, low = split(edge * w)
            ring[2 * i * RING : (2 * i + 1) * RING, :] = high
            ring[(2 * i + 1) * RING : (2 * i + 2) * RING, :] = low
            high, low = split(core * w)
            inner[2 * i * CORE : (2 * i + 1) * CORE, pl.ds(at, width)] = high
            inner[(2 * i + 1) * CORE : (2 * i + 2) * CORE, pl.ds(at, width)] = low
        number = lax.broadcasted_iota(jnp.int32, (slots, cells * depth), 1).astype(F32)
        for i in range(TILES):
            ident = tiles[i].T[:, 7:8]
            hot[pl.ds(at + i * slots, slots), :] = jnp.where(number == ident, 1.0, 0.0).astype(BF16)

    def gather_ring(ring, hot, at):
        for cell in range(cells):
            r = dot(ring[...], hot[pl.ds(at, width), cell * depth : (cell + 1) * depth])
            for i in range(3):
                acc[cell, i * PAD : i * PAD + RING, :] += (
                    r[2 * i * RING : (2 * i + 1) * RING]
                    + r[(2 * i + 1) * RING : (2 * i + 2) * RING]
                )

    def gather_core(cell):
        where = slice(cell * depth, (cell + 1) * depth)
        r = dot(in_a[...], hot_a[:, where]) + dot(in_b[...], hot_b[:, where])
        return [
            acc[cell, i * PAD + RING : (i + 1) * PAD, :]
            + r[2 * i * CORE : (2 * i + 1) * CORE]
            + r[(2 * i + 1) * CORE : (2 * i + 2) * CORE]
            for i in range(3)
        ]

    def inject(first, last):
        wait_tiles(first, TILES)
        prepare(first, lhs_a, in_a, hot_a, 0)

        def pair(j, carry):
            one, two = first + (2 * j + 1) * TILES, first + (2 * j + 2) * TILES
            wait_tiles(one, TILES)
            here = pl.multiple_of(j * width, width)
            then = pl.multiple_of((j + 1) * width, width)
            prepare(one, lhs_b, in_b, hot_b, here)
            gather_ring(lhs_a, hot_a, here)
            wait_tiles(two, TILES)
            prepare(two, lhs_a, in_a, hot_a, then)
            gather_ring(lhs_b, hot_b, here)
            return carry

        half = chunks // 2
        lax.fori_loop(0, half - 1, pair, 0)
        end = first + (chunks - 1) * TILES
        wait_tiles(end, TILES - 1 if last else TILES)
        prepare(end, lhs_b, in_b, hot_b, (half - 1) * width)
        gather_ring(lhs_a, hot_a, (half - 1) * width)
        gather_ring(lhs_b, hot_b, (half - 1) * width)

    if n > span:
        def early(b, carry):
            inject(b * span + 1, False)
            for cell in range(cells):
                for i, f in enumerate(gather_core(cell)):
                    acc[cell, i * PAD + RING : (i + 1) * PAD, :] = f
            return carry

        lax.fori_loop(0, n // span - 1, early, 0)
    inject(n - span + 1, True)

    def stitch(low, high):
        lane = lax.broadcasted_iota(jnp.int32, low.shape, 1)
        up = jnp.where(lane < depth - 1, pltpu.roll(low, depth - 1, 1), 0.0)
        down = jnp.where(lane > 0, pltpu.roll(high, 1, 1), 0.0)
        return low + down, high + up

    def join(a, ra, b, rb, size):
        total = acc[a, ra : ra + size, :] + acc[b, rb : rb + size, :]
        acc[a, ra : ra + size, :] = total
        acc[b, rb : rb + size, :] = total

    def there(m):
        return neighbour(m, gx, gy, nx, ny)

    quad = 4 * halves
    line = (4 * cx - 1) * quad
    last = slice(depth - 128, depth)

    def strip_copy(src, dst, m, slot, where):
        dx, dy = MOVES[m]
        side, other = m % 2, 1 - m % 2
        return pltpu.make_async_remote_copy(
            src_ref=src.at[(side,) + where],
            dst_ref=dst.at[(other,) + where],
            send_sem=halo_send.at[2 * slot + m],
            recv_sem=halo_recv.at[2 * slot + m],
            device_id=(gx + dx, gy + dy),
            device_id_type=MESH,
        )

    def arriving(src, dst, m, slot, where):
        dx, dy = MOVES[m]
        return pltpu.make_async_remote_copy(
            src_ref=src.at[(m % 2,) + where],
            dst_ref=dst.at[(m % 2,) + where],
            send_sem=halo_send.at[2 * slot + m],
            recv_sem=halo_recv.at[2 * slot + m + 1 - 2 * (m % 2)],
            device_id=(gx + dx, gy + dy),
            device_id_type=MESH,
        )

    def part(c):
        return (pl.ds(c * line, line + (quad if c == 2 else 0)),)

    def pack_tips(rows):
        lane = lax.broadcasted_iota(jnp.int32, rows[0].shape, 1)
        total = rows[0]
        for c in (1, 2):
            total = jnp.where(lane == 127 - c, pltpu.roll(rows[c], 128 - c, 1), total)
        return total

    for c in range(3):
        o = c * PAD
        for cell in range(cells):
            low, high = stitch(acc[cell, o : o + 16, :], acc[cell, o + 64 : o + 80, :])
            acc[cell, o : o + 16, :] = low
            acc[cell, o + 64 : o + 80, :] = high
        for r in range(5):
            k = o + r * 16
            for y in range(cy):
                for x in range(cx - 1):
                    join(x * cy + y, k + 8, (x + 1) * cy + y, k, 5)
            for x in range(cx):
                for y in range(cy - 1):
                    a, b = x * cy + y, x * cy + y + 1
                    join(a, k + 13, b, k + 5, 3)
                    join(a, k + 4, b, k, 1)
                    join(a, k + 12, b, k + 8, 1)
        for y in range(cy):
            for side in (0, 1):
                cell = side * (cx - 1) * cy + y
                for h in range(halves):
                    for r in range(5):
                        k = o + r * 16 + side * 8
                        xs[side, c, pl.ds(r * rows_node + h * cy + y, 5, stride=5 * rows_node), :] = (
                            acc[cell, k : k + 5, h * 128 : (h + 1) * 128]
                        )
        for m in (0, 1):
            @pl.when(there(m))
            def _():
                strip_copy(xs, rx, m, 0, (c,)).start()
        for side in (0, 1):
            low, mid, high = ((0, 5, 8), (4, 13, 12))[side]
            for x in range(cx):
                cell = x * cy + side * (cy - 1)
                for r in range(4):
                    k = o + r * 16
                    for h in range(halves):
                        lanes = slice(h * 128, (h + 1) * 128)
                        to = r * halves + h
                        at = c * line + x * 4 * quad + to
                        ys[side, pl.ds(at, 3, stride=quad), :] = acc[
                            cell, k + mid : k + mid + 3, lanes
                        ]
                        if x < cx - 1:
                            ys[side, at + 3 * quad : at + 3 * quad + 1, :] = acc[
                                cell, k + high : k + high + 1, lanes
                            ]
                        for e, row in ((0, low), (1, high)):
                            if x == e * (cx - 1):
                                at_e = (c * 2 + e) * quad + to
                                es[side, at_e : at_e + 1, :] = acc[
                                    cell, k + row : k + row + 1, lanes
                                ]
                k = o + 64
                tips[side, c, x * 4 : x * 4 + 3, :] = acc[cell, k + mid : k + mid + 3, last]
                for e, row in ((0, low), (1, high)):
                    if x == e * (cx - 1):
                        tips[2 + side, c, e : e + 1, :] = acc[cell, k + row : k + row + 1, last]
                if x < cx - 1:
                    tips[side, c, x * 4 + 3 : x * 4 + 4, :] = acc[cell, k + high : k + high + 1, last]
            if c == 2:
                ys[side, 3 * line : 3 * line + quad, :] = pack_tips([tips[side, d] for d in range(3)])
        for m in (2, 3):
            @pl.when(there(m))
            def _():
                strip_copy(ys, ry, m, 0, part(c)).start()

    def place_rows(cell, c, values, row, size, node, step):
        start = ((cell // cy) * 3 + c) * 125 * rows_node + cell % cy
        for h in range(halves):
            at = start + h * cy + node * rows_node
            part = values[row : row + size, h * 128 : (h + 1) * 128]
            pre_h[pl.ds(at, size, stride=step * rows_node), :] = part

    def fold_edges():
        for m in (0, 1):
            @pl.when(there(m))
            def _():
                arriving(xs, rx, m, 0, ()).wait_recv()
                for c in range(3):
                    for side in (0, 1):
                        at = side * (20 * rows_node + cy - 1)
                        k = (c * 2 + m) * quad
                        es[side, k : k + quad, :] += rx[m, c, pl.ds(at, quad, stride=cy), :]
                        tip = at + 4 * rows_node + (halves - 1) * cy
                        tips[2 + side, c, m : m + 1, :] += rx[m, c, tip : tip + 1, :]

        for side in (0, 1):
            es[side, 6 * quad : 7 * quad, :] = pack_tips([tips[2 + side, d] for d in range(3)])
            m = 2 + side

            @pl.when(there(m))
            def _():
                strip_copy(es, re, m, 1, ()).start()

    for x in range(cx):
        if x == cx - 1:
            fold_edges()
        for y in range(cy):
            cell = x * cy + y
            inner = gather_core(cell)
            for c in range(3):
                f = inner[c]
                low, high = stitch(f[0:8], f[32:40])
                lane = lax.broadcasted_iota(jnp.int32, (8, depth), 1)
                row = lax.broadcasted_iota(jnp.int32, (8, depth), 0)
                tail = f[40:48]
                up = pltpu.roll(pltpu.roll(tail, depth - 1, 1), 4, 0)
                down = pltpu.roll(pltpu.roll(tail, 1, 1), 4, 0)
                tail = (
                    tail
                    + jnp.where((row == 4) & (lane < depth - 1), up, 0.0)
                    + jnp.where((row == 0) & (lane > 0), down, 0.0)
                )
                planes = [low, f[8:16], f[16:24], f[24:32], high]
                for r in range(5):
                    ring = acc[cell, c * PAD + r * 16 : c * PAD + r * 16 + 16, :]
                    place_rows(cell, c, ring, 0, 5, r, 5)
                    place_rows(cell, c, ring, 5, 3, 25 + r, 25)
                    place_rows(cell, c, ring, 8, 5, 100 + r, 5)
                    place_rows(cell, c, ring, 13, 3, 45 + r, 25)
                    place_rows(cell, c, planes[r], 0, 3, 30 + r, 5)
                    place_rows(cell, c, planes[r], 3, 3, 55 + r, 5)
                    place_rows(cell, c, planes[r], 6, 2, 80 + r, 5)
                place_rows(cell, c, tail, 0, 5, 90, 1)

    many(n - 1, 0).wait_send()
    for m in (0, 1):
        @pl.when(there(m))
        def _():
            strip_copy(xs, rx, m, 0, ()).wait_send()

    for m in (2, 3):
        @pl.when(there(m))
        def _():
            arriving(ys, ry, m, 0, ()).wait_recv()
            strip_copy(ys, ry, m, 0, ()).wait_send()
            arriving(es, re, m, 1, ()).wait_recv()
            strip_copy(es, re, m, 1, ()).wait_send()


def finish_kernel(cx, cy, pre, rx, ry, re, out_h, buf, out_sem):
    total = buf.shape[0]
    block = total // (cx * 3)
    rows_node = block // 125
    halves = rows_node // cy
    plane, quad = 25 * rows_node, 4 * halves
    line = (4 * cx - 1) * quad
    lane = lax.broadcasted_iota(jnp.int32, (quad, 128), 1)
    row = lax.broadcasted_iota(jnp.int32, (quad, 128), 0)
    copies, done = [], 0
    for k in range(cx * 3):
        x, c = k // 3, k % 3
        base = k * block
        buf[base : base + block, :] = pre[base : base + block, :]
        if x == 0:
            buf[base : base + plane, :] += rx[0, c, :plane]
        if x == cx - 1:
            buf[base + 4 * plane : base + 5 * plane, :] += rx[1, c, :plane]
        for side in (0, 1):
            tips = pltpu.roll(ry[side, 3 * line : 3 * line + quad, :], c, 1)
            ends = pltpu.roll(re[side, 6 * quad : 7 * quad, :], c, 1)
            for p in range(5):
                pp = x * 4 + p
                if pp % (4 * cx) == 0:
                    e = pp // (4 * cx)
                    at = (c * 2 + e) * quad
                    values, tip = re[side, at : at + quad, :], ends[e : e + 1]
                else:
                    at = c * line + (pp - 1) * quad
                    values, tip = ry[side, at : at + quad, :], tips[pp - 1 : pp]
                ahead = pltpu.roll(values, 127, 1)
                beyond = jnp.where(row == halves - 1, tip, pltpu.roll(ahead, quad - 1, 0))
                upper = jnp.where(lane < 127, ahead, beyond)
                to = base + (p * 25 + side * 20) * rows_node + side * (cy - 1)
                buf[pl.ds(to, quad, stride=cy), :] += values
                buf[pl.ds(to + quad * cy, halves, stride=cy), :] += upper[:halves]
        upto = (k + 1) * block // 8 * 8
        copy = pltpu.make_async_copy(
            buf.at[pl.ds(done, upto - done)], out_h.at[pl.ds(done, upto - done)], out_sem.at[k]
        )
        copy.start()
        copies.append(copy)
        done = upto
    for copy in copies:
        copy.wait()


def anywhere(count):
    return [pl.BlockSpec(memory_space=pl.ANY)] * count


def body(nx, ny, wavefield, moduli, residuals, coords, angles, element_ids, counts):
    cx, cy, depth = wavefield.shape[0], wavefield.shape[1], wavefield.shape[4]
    n, slots = nx * ny, residuals.shape[2]
    cells, halves = cx * cy, depth // 128
    span = min(n, SPAN)
    width = TILES * slots
    rows = wavefield.transpose(0, 2, 3, 1, 4).reshape(cx, 3, 125, cy, halves, 128)
    rows = rows.transpose(0, 1, 2, 4, 3, 5).reshape(-1, 128)
    coords = coords.transpose(0, 2, 1, 3)
    moduli = moduli.reshape(cells, 2, depth)
    operands = [residuals, coords, angles, element_ids, counts, rows, moduli, *tables()]
    quad = 4 * halves
    received = [
        (2, 3, -(-25 * halves * cy // 8) * 8, 128),
        (2, 3 * (4 * cx - 1) * quad + quad, 128),
        (2, 7 * quad, 128),
    ]
    scratch = [pltpu.VMEM(a.shape, a.dtype) for a in operands]
    scratch += [
        pltpu.VMEM((n, 8, slots), F32),
        pltpu.VMEM((n, 8, slots), F32),
        pltpu.VMEM((cells, 3 * PAD, depth), F32),
        pltpu.VMEM((6 * RING, width), BF16),
        pltpu.VMEM((6 * RING, width), BF16),
        pltpu.VMEM((6 * CORE, span * slots // 2), BF16),
        pltpu.VMEM((6 * CORE, span * slots // 2), BF16),
        pltpu.VMEM((span * slots // 2, cells * depth), BF16),
        pltpu.VMEM((span * slots // 2, cells * depth), BF16),
        pltpu.VMEM((2, 3, PAD, depth), F32),
    ]
    scratch += [pltpu.VMEM(s, F32) for s in received + [(4, 3, quad, 128)]]
    scratch += [
        pltpu.SemaphoreType.DMA((len(operands),)),
        pltpu.SemaphoreType.DMA((1,)),
        pltpu.SemaphoreType.DMA((n // TILES,)),
        pltpu.SemaphoreType.DMA((6,)),
        pltpu.SemaphoreType.DMA((6,)),
    ]
    parts = pl.pallas_call(
        functools.partial(step_kernel, nx, ny, cx, cy),
        out_shape=[pltpu.VMEM(s, F32) for s in [rows.shape] + received],
        in_specs=anywhere(len(operands)),
        out_specs=[pl.BlockSpec(memory_space=pltpu.VMEM)] * 4,
        scratch_shapes=scratch,
        compiler_params=pltpu.CompilerParams(collective_id=0, has_side_effects=True, vmem_limit_bytes=48 << 20),
    )(*[pltpu.with_memory_space_constraint(a, pltpu.HBM) for a in operands])
    force = pl.pallas_call(
        functools.partial(finish_kernel, cx, cy),
        out_shape=jax.ShapeDtypeStruct(rows.shape, F32),
        in_specs=[pl.BlockSpec(memory_space=pltpu.VMEM)] * 4,
        out_specs=anywhere(1)[0],
        scratch_shapes=[pltpu.VMEM(rows.shape, F32), pltpu.SemaphoreType.DMA((cx * 3,))],
        compiler_params=pltpu.CompilerParams(vmem_limit_bytes=16 << 20),
    )(*parts)
    force = force.reshape(cx, 3, 125, halves, cy, 128).transpose(0, 1, 2, 4, 3, 5)
    return force.reshape(cx, 3, 125, cy, depth).transpose(0, 3, 1, 2, 4)


def solution(mesh):
    in_specs = (
        P("gx", "gy", None, None, None),
        P("gx", "gy", None, None),
        P(("gx", "gy"), None, None),
        P(("gx", "gy"), None, None, None),
        P(("gx", "gy"), None, None, None),
        P(("gx", "gy"), None, None),
        P(("gx", "gy"), None),
    )
    out_specs = P("gx", "gy", None, None, None)
    return jax.shard_map(
        functools.partial(body, mesh.shape["gx"], mesh.shape["gy"]),
        mesh=mesh,
        in_specs=in_specs,
        out_specs=out_specs,
        check_vma=False,
    )
```

```python
import functools
import math

import jax
import jax.numpy as jnp
import numpy as np
from jax import lax
from jax.experimental import pallas as pl
from jax.experimental.pallas import tpu as pltpu
from jax.sharding import PartitionSpec as P

MESH = pl.DeviceIdType.MESH
F32, BF16 = jnp.float32, jnp.bfloat16
PAD = 128
SPAN = 32
TILES = 4
RING, CORE = 80, 48

EDGE = [(0, 0), (0, 1), (0, 2), (0, 3), (0, 4), (1, 0), (2, 0), (3, 0)]
EDGE += [(4, 0), (4, 1), (4, 2), (4, 3), (4, 4), (1, 4), (2, 4), (3, 4)]
INNER = [(1, 1), (1, 2), (1, 3), (2, 1), (2, 2), (2, 3), (3, 1), (3, 2)]
LAST = (3, 3)


def node_order():
    order = []
    for r in range(5):
        order += [(p * 5 + q) * 5 + r for p, q in EDGE]
    for r in range(5):
        order += [(p * 5 + q) * 5 + r for p, q in INNER]
    order += [(LAST[0] * 5 + LAST[1]) * 5 + r for r in range(5)]
    return np.array(order)


def gll_points():
    return np.array([-1.0, -math.sqrt(3.0 / 7.0), 0.0, math.sqrt(3.0 / 7.0), 1.0])


def gll_weights():
    return np.array([0.1, 49.0 / 90.0, 32.0 / 45.0, 49.0 / 90.0, 0.1])


def derivative_table():
    points = gll_points()
    table = np.zeros((5, 5))
    for row in range(5):
        for col in range(5):
            if row == col:
                table[row, col] = sum(
                    (1.0 / (points[col] - points[other]) for other in range(5) if other != col)
                )
            else:
                value = 1.0 / (points[col] - points[row])
                for other in range(5):
                    if other != col and other != row:
                        value = (
                            value * (points[row] - points[other]) / (points[col] - points[other])
                        )
                table[row, col] = value
    return table


def split_table(table):
    high = table.astype(BF16)
    return high, (table - high.astype(np.float64)).astype(BF16)


def roots(k):
    points = gll_points()
    others = [m for m in range(5) if m != k]
    return [points[m] for m in others], 1.0 / np.prod([points[k] - points[m] for m in others])


def tables():
    dm, eye = derivative_table(), np.eye(5)
    w1 = gll_weights()
    weight = (w1[:, None, None] * w1[None, :, None] * w1[None, None, :]).reshape(-1)
    dirs = [
        np.kron(np.kron(dm, eye), eye),
        np.kron(np.kron(eye, dm), eye),
        np.kron(np.kron(eye, eye), dm),
    ]
    order = node_order()
    grad = np.zeros((3 * PAD, PAD))
    back = np.zeros((PAD, 3 * PAD))
    for j in range(3):
        grad[j * PAD : j * PAD + 125, :125] = dirs[j][order]
        full = -dirs[j].T * weight[None, :]
        back[:125, j * PAD : j * PAD + 125] = full[order][:, order]
    gh, gl = split_table(grad)
    bh, bl = split_table(back)
    g1 = np.concatenate([gh, gh], 1)
    bs = np.concatenate([bh, bl], 0)
    consts = np.zeros((41, 8, 128), np.float32)
    for g, group in enumerate((EDGE[:8], EDGE[8:], INNER, [LAST] * 8)):
        for row, (p, q) in enumerate(group):
            rp, sp = roots(p)
            rq, sq = roots(q)
            for j in range(4):
                consts[g * 9 + j, row] = rp[j]
                consts[g * 9 + 4 + j, row] = rq[j]
            consts[g * 9 + 8, row] = sp * sq
    for r in range(5):
        rr, sr = roots(r)
        for j in range(4):
            consts[36 + j, r] = rr[j]
        consts[40, r] = sr
    return jnp.asarray(g1), jnp.asarray(gl), jnp.asarray(bs), jnp.asarray(consts)


def split(x):
    high = x.astype(BF16)
    return high, (x - high.astype(F32)).astype(BF16)


def dot(a, b):
    return jnp.dot(a, b, preferred_element_type=F32)


def sin_cos(x):
    h = x * 0.5
    h2 = h * h
    s = c = None
    for k in range(6, -1, -1):
        a = (-1.0) ** k / math.factorial(2 * k + 1)
        b = (-1.0) ** k / math.factorial(2 * k)
        s = jnp.full(x.shape, a, F32) if s is None else s * h2 + a
        c = jnp.full(x.shape, b, F32) if c is None else c * h2 + b
    s = s * h
    return 2.0 * s * c, 1.0 - 2.0 * s * s


def quartic(x, rows):
    a, b, c, d = [x - row for row in rows]
    ab, cd = a * b, c * d
    return ab * cd, (a + b) * cd + ab * (c + d)


MOVES = [(-1, 0), (1, 0), (0, -1), (0, 1)]


def neighbour(m, gx, gy, nx, ny):
    step = MOVES[m][m // 2]
    pos, total = ((gx, nx), (gy, ny))[m // 2]
    return pos > 0 if step < 0 else pos < total - 1


def step_kernel(
    nx, ny, cx, cy, resid_h, coord_h, angle_h, ids_h, count_h, u_h, mod_h, g1_h, g2_h, bs_h,
    consts_h, pre_h, rx, ry, re,
    resid, coord, angle, ids, count, u_ref, mod_ref, g1, g2, bs, consts,
    packed, got, acc, lhs_a, lhs_b, in_a, in_b, hot_a, hot_b, pad, xs, ys, es, tips,
    load_sem, send_sem, recv_sem, halo_send, halo_recv,
):
    n = nx * ny
    gx, gy = lax.axis_index("gx"), lax.axis_index("gy")
    me = gx * ny + gy
    cells, depth, slots = cx * cy, acc.shape[2], resid.shape[2]
    halves = depth // 128
    rows_node = halves * cy
    span = min(n, SPAN)
    chunks = span // TILES
    width = TILES * slots
    barrier = pltpu.get_barrier_semaphore()

    def after(k):
        to = me + k
        to = jnp.where(to >= n, to - n, to)
        return to, (lax.div(to, ny), lax.rem(to, ny))

    def greet(k):
        pl.semaphore_signal(barrier, inc=1, device_id=after(k)[1], device_id_type=MESH)

    def repeat(action):
        if n <= SPAN:
            for k in range(1, n):
                action(k)
        else:
            def one(k, c):
                action(k)
                return c

            lax.fori_loop(1, n, one, 0)

    pairs = [
        (count_h, count), (angle_h, angle), (resid_h, resid), (coord_h, coord), (ids_h, ids),
        (u_h, u_ref), (mod_h, mod_ref), (g1_h, g1), (g2_h, g2), (bs_h, bs), (consts_h, consts),
    ]
    loads = [pltpu.make_async_copy(a, b, load_sem.at[k]) for k, (a, b) in enumerate(pairs)]
    for copy in loads:
        copy.start()
    repeat(greet)
    for copy in loads[:5]:
        copy.wait()

    rows = lax.broadcasted_iota(jnp.int32, (n, n), 0)
    cols = lax.broadcasted_iota(jnp.int32, (n, n), 1)
    diagonal = jnp.where(rows == cols, count[...].astype(F32), 0.0)
    live_count = jnp.sum(diagonal, axis=1, keepdims=True)
    slot = lax.broadcasted_iota(jnp.int32, (n, slots), 1).astype(F32)
    sa, ca = sin_cos(angle[0, :, 0, :])
    sd, cd = sin_cos(angle[0, :, 1, :])
    packed[:, 0, :] = jnp.where(slot < live_count, resid[0], 0.0)
    for d in range(3):
        packed[:, 1 + d, :] = coord[0, d]
    packed[:, 4, :] = ca * cd
    packed[:, 5, :] = sa * cd
    packed[:, 6, :] = sd
    packed[:, 7, :] = ids[0].astype(F32)
    tips[...] = jnp.zeros_like(tips)
    for m in range(4):
        @pl.when(jnp.logical_not(neighbour(m, gx, gy, nx, ny)))
        def _():
            for hole in ((rx,), (ry, re))[m // 2]:
                hole[m % 2] = jnp.zeros(hole.shape[1:], F32)

    def strain(cell, slab, c):
        start = ((cell // cy) * 3 + c) * 125 * rows_node + cell % cy
        for h in range(halves):
            pad[slab, c, 0:125, h * 128 : (h + 1) * 128] = u_ref[
                pl.ds(start + h * cy, 125, stride=rows_node), :
            ]
        high, low = split(pad[slab, c])
        r = dot(g1[...], jnp.concatenate([high, low], axis=0)) + dot(g2[...], high)
        return [r[j * PAD : (j + 1) * PAD] for j in range(3)]

    def stiff(group):
        g = {cell: [] for cell in group}
        for c in range(3):
            for cell in group:
                g[cell].append(strain(cell, cell % len(group), c))
        press = {}
        for cell in group:
            press[cell] = mod_ref[cell, 0:1, :] * (g[cell][0][0] + g[cell][1][1] + g[cell][2][2])
        for i in range(3):
            for cell in group:
                mu, parts = mod_ref[cell, 1:2, :], []
                for j in range(3):
                    s = mu * (g[cell][i][j] + g[cell][j][i])
                    parts.append(s + press[cell] if i == j else s)
                high, low = split(jnp.concatenate(parts, axis=0))
                r = dot(bs[...], high)
                acc[cell, i * PAD : (i + 1) * PAD, :] = r[:PAD] + r[PAD:] + dot(bs[:PAD], low)

    pl.semaphore_wait(barrier, n - 1)

    def tile_copy(k, at):
        to, where = after(k)
        return pltpu.make_async_remote_copy(
            src_ref=packed.at[to],
            dst_ref=got.at[at],
            send_sem=send_sem.at[0],
            recv_sem=recv_sem.at[(k - 1) // TILES],
            device_id=where,
            device_id_type=MESH,
        )

    def send(k):
        tile_copy(k, me).start()

    repeat(send)
    got[me] = packed[me]
    pad[:, :, PAD - 8 :, :] = jnp.zeros((cells, 3, 8, depth), F32)
    for copy in loads[5:]:
        copy.wait()
    stiff(range(cells))

    def many(count, group):
        other = lax.rem(me + 1, n)
        return pltpu.make_async_remote_copy(
            src_ref=packed.at[pl.ds(0, count)],
            dst_ref=got.at[pl.ds(0, count)],
            send_sem=send_sem.at[0],
            recv_sem=recv_sem.at[group],
            device_id=(other // ny, lax.rem(other, ny)),
            device_id_type=MESH,
        )

    def wait_tiles(first, count):
        many(count, (first - 1) // TILES).wait_recv()

    def prepare(first, ring, inner, hot, at):
        tiles = [got[lax.rem(me - (first + i) + n, n)] for i in range(TILES)]
        tile = jnp.concatenate(tiles, axis=1)

        def const(k):
            return jnp.concatenate([consts[k]] * TILES, axis=1)

        v = tile[0:1]
        t = [tile[4 + i : 5 + i] for i in range(3)]
        x, y, z = [jnp.broadcast_to(tile[1 + d : 2 + d], (8, width)) for d in range(3)]
        lz, dz = quartic(z, [const(36 + j) for j in range(4)])
        lz, dz = lz * const(40), dz * (const(40) * t[2])
        first_of, second_of = [], []
        for g in range(4):
            lx, dx = quartic(x, [const(g * 9 + j) for j in range(4)])
            ly, dy = quartic(y, [const(g * 9 + 4 + j) for j in range(4)])
            scale = const(g * 9 + 8)
            first_of.append(scale * ((t[0] * dx) * ly + (t[1] * dy) * lx))
            second_of.append(scale * (lx * ly))
        edge, core = [], []
        for r in range(5):
            a = jnp.broadcast_to(lz[r : r + 1], (8, width))
            b = jnp.broadcast_to(dz[r : r + 1], (8, width))
            edge += [first_of[g] * a + second_of[g] * b for g in (0, 1)]
            core.append(first_of[2] * a + second_of[2] * b)
        core.append(first_of[3] * lz + second_of[3] * dz)
        edge, core = jnp.concatenate(edge, axis=0), jnp.concatenate(core, axis=0)
        for i in range(3):
            w = v * t[i]
            high, low = split(edge * w)
            ring[2 * i * RING : (2 * i + 1) * RING, :] = high
            ring[(2 * i + 1) * RING : (2 * i + 2) * RING, :] = low
            high, low = split(core * w)
            inner[2 * i * CORE : (2 * i + 1) * CORE, pl.ds(at, width)] = high
            inner[(2 * i + 1) * CORE : (2 * i + 2) * CORE, pl.ds(at, width)] = low
        number = lax.broadcasted_iota(jnp.int32, (slots, cells * depth), 1).astype(F32)
        for i in range(TILES):
            ident = tiles[i].T[:, 7:8]
            hot[pl.ds(at + i * slots, slots), :] = jnp.where(number == ident, 1.0, 0.0).astype(BF16)

    def gather_ring(ring, hot, at):
        for cell in range(cells):
            r = dot(ring[...], hot[pl.ds(at, width), cell * depth : (cell + 1) * depth])
            for i in range(3):
                acc[cell, i * PAD : i * PAD + RING, :] += (
                    r[2 * i * RING : (2 * i + 1) * RING]
                    + r[(2 * i + 1) * RING : (2 * i + 2) * RING]
                )

    def gather_core(cell):
        where = slice(cell * depth, (cell + 1) * depth)
        r = dot(in_a[...], hot_a[:, where]) + dot(in_b[...], hot_b[:, where])
        return [
            acc[cell, i * PAD + RING : (i + 1) * PAD, :]
            + r[2 * i * CORE : (2 * i + 1) * CORE]
            + r[(2 * i + 1) * CORE : (2 * i + 2) * CORE]
            for i in range(3)
        ]

    def inject(first, last):
        wait_tiles(first, TILES)
        prepare(first, lhs_a, in_a, hot_a, 0)

        def pair(j, carry):
            one, two = first + (2 * j + 1) * TILES, first + (2 * j + 2) * TILES
            wait_tiles(one, TILES)
            here = pl.multiple_of(j * width, width)
            then = pl.multiple_of((j + 1) * width, width)
            prepare(one, lhs_b, in_b, hot_b, here)
            gather_ring(lhs_a, hot_a, here)
            wait_tiles(two, TILES)
            prepare(two, lhs_a, in_a, hot_a, then)
            gather_ring(lhs_b, hot_b, here)
            return carry

        half = chunks // 2
        lax.fori_loop(0, half - 1, pair, 0)
        end = first + (chunks - 1) * TILES
        wait_tiles(end, TILES - 1 if last else TILES)
        prepare(end, lhs_b, in_b, hot_b, (half - 1) * width)
        gather_ring(lhs_a, hot_a, (half - 1) * width)
        gather_ring(lhs_b, hot_b, (half - 1) * width)

    if n > span:
        def early(b, carry):
            inject(b * span + 1, False)
            for cell in range(cells):
                for i, f in enumerate(gather_core(cell)):
                    acc[cell, i * PAD + RING : (i + 1) * PAD, :] = f
            return carry

        lax.fori_loop(0, n // span - 1, early, 0)
    inject(n - span + 1, True)

    def stitch(low, high):
        lane = lax.broadcasted_iota(jnp.int32, low.shape, 1)
        up = jnp.where(lane < depth - 1, pltpu.roll(low, depth - 1, 1), 0.0)
        down = jnp.where(lane > 0, pltpu.roll(high, 1, 1), 0.0)
        return low + down, high + up

    def join(a, ra, b, rb, size):
        total = acc[a, ra : ra + size, :] + acc[b, rb : rb + size, :]
        acc[a, ra : ra + size, :] = total
        acc[b, rb : rb + size, :] = total

    def there(m):
        return neighbour(m, gx, gy, nx, ny)

    quad = 4 * halves
    line = (4 * cx - 1) * quad
    last = slice(depth - 128, depth)

    def strip_copy(src, dst, m, slot, where):
        dx, dy = MOVES[m]
        side, other = m % 2, 1 - m % 2
        return pltpu.make_async_remote_copy(
            src_ref=src.at[(side,) + where],
            dst_ref=dst.at[(other,) + where],
            send_sem=halo_send.at[2 * slot + m],
            recv_sem=halo_recv.at[2 * slot + m],
            device_id=(gx + dx, gy + dy),
            device_id_type=MESH,
        )

    def arriving(src, dst, m, slot, where):
        dx, dy = MOVES[m]
        return pltpu.make_async_remote_copy(
            src_ref=src.at[(m % 2,) + where],
            dst_ref=dst.at[(m % 2,) + where],
            send_sem=halo_send.at[2 * slot + m],
            recv_sem=halo_recv.at[2 * slot + m + 1 - 2 * (m % 2)],
            device_id=(gx + dx, gy + dy),
            device_id_type=MESH,
        )

    def part(c):
        return (pl.ds(c * line, line + (quad if c == 2 else 0)),)

    def pack_tips(rows):
        lane = lax.broadcasted_iota(jnp.int32, rows[0].shape, 1)
        total = rows[0]
        for c in (1, 2):
            total = jnp.where(lane == 127 - c, pltpu.roll(rows[c], 128 - c, 1), total)
        return total

    for c in range(3):
        o = c * PAD
        for cell in range(cells):
            low, high = stitch(acc[cell, o : o + 16, :], acc[cell, o + 64 : o + 80, :])
            acc[cell, o : o + 16, :] = low
            acc[cell, o + 64 : o + 80, :] = high
        for r in range(5):
            k = o + r * 16
            for y in range(cy):
                for x in range(cx - 1):
                    join(x * cy + y, k + 8, (x + 1) * cy + y, k, 5)
            for x in range(cx):
                for y in range(cy - 1):
                    a, b = x * cy + y, x * cy + y + 1
                    join(a, k + 13, b, k + 5, 3)
                    join(a, k + 4, b, k, 1)
                    join(a, k + 12, b, k + 8, 1)
        for side in (0, 1):
            low, mid, high = ((0, 5, 8), (4, 13, 12))[side]
            for x in range(cx):
                cell = x * cy + side * (cy - 1)
                for r in range(4):
                    k = o + r * 16
                    for h in range(halves):
                        lanes = slice(h * 128, (h + 1) * 128)
                        to = r * halves + h
                        at = c * line + x * 4 * quad + to
                        ys[side, pl.ds(at, 3, stride=quad), :] = acc[
                            cell, k + mid : k + mid + 3, lanes
                        ]
                        if x < cx - 1:
                            ys[side, at + 3 * quad : at + 3 * quad + 1, :] = acc[
                                cell, k + high : k + high + 1, lanes
                            ]
                        for e, row in ((0, low), (1, high)):
                            if x == e * (cx - 1):
                                at_e = (c * 2 + e) * quad + to
                                es[side, at_e : at_e + 1, :] = acc[
                                    cell, k + row : k + row + 1, lanes
                                ]
                k = o + 64
                tips[side, c, x * 4 : x * 4 + 3, :] = acc[cell, k + mid : k + mid + 3, last]
                for e, row in ((0, low), (1, high)):
                    if x == e * (cx - 1):
                        tips[2 + side, c, e : e + 1, :] = acc[cell, k + row : k + row + 1, last]
                if x < cx - 1:
                    tips[side, c, x * 4 + 3 : x * 4 + 4, :] = acc[cell, k + high : k + high + 1, last]
            if c == 2:
                ys[side, 3 * line : 3 * line + quad, :] = pack_tips([tips[side, d] for d in range(3)])
        for m in (2, 3):
            @pl.when(there(m))
            def _():
                strip_copy(ys, ry, m, 0, part(c)).start()
        for y in range(cy):
            for side in (0, 1):
                cell = side * (cx - 1) * cy + y
                for h in range(halves):
                    for r in range(5):
                        k = o + r * 16 + side * 8
                        xs[side, c, pl.ds(r * rows_node + h * cy + y, 5, stride=5 * rows_node), :] = (
                            acc[cell, k : k + 5, h * 128 : (h + 1) * 128]
                        )
        for m in (0, 1):
            @pl.when(there(m))
            def _():
                strip_copy(xs, rx, m, 0, (c,)).start()

    def place_rows(cell, c, values, row, size, node, step):
        start = ((cell // cy) * 3 + c) * 125 * rows_node + cell % cy
        for h in range(halves):
            at = start + h * cy + node * rows_node
            part = values[row : row + size, h * 128 : (h + 1) * 128]
            pre_h[pl.ds(at, size, stride=step * rows_node), :] = part

    def fold_edges():
        for m in (0, 1):
            @pl.when(there(m))
            def _():
                arriving(xs, rx, m, 0, ()).wait_recv()
                for c in range(3):
                    for side in (0, 1):
                        at = side * (20 * rows_node + cy - 1)
                        k = (c * 2 + m) * quad
                        es[side, k : k + quad, :] += rx[m, c, pl.ds(at, quad, stride=cy), :]
                        tip = at + 4 * rows_node + (halves - 1) * cy
                        tips[2 + side, c, m : m + 1, :] += rx[m, c, tip : tip + 1, :]

        for side in (0, 1):
            es[side, 6 * quad : 7 * quad, :] = pack_tips([tips[2 + side, d] for d in range(3)])
            m = 2 + side

            @pl.when(there(m))
            def _():
                strip_copy(es, re, m, 1, ()).start()

    for x in range(cx):
        if x == cx - 1:
            fold_edges()
        for y in range(cy):
            cell = x * cy + y
            inner = gather_core(cell)
            for c in range(3):
                f = inner[c]
                low, high = stitch(f[0:8], f[32:40])
                lane = lax.broadcasted_iota(jnp.int32, (8, depth), 1)
                row = lax.broadcasted_iota(jnp.int32, (8, depth), 0)
                tail = f[40:48]
                up = pltpu.roll(pltpu.roll(tail, depth - 1, 1), 4, 0)
                down = pltpu.roll(pltpu.roll(tail, 1, 1), 4, 0)
                tail = (
                    tail
                    + jnp.where((row == 4) & (lane < depth - 1), up, 0.0)
                    + jnp.where((row == 0) & (lane > 0), down, 0.0)
                )
                planes = [low, f[8:16], f[16:24], f[24:32], high]
                for r in range(5):
                    ring = acc[cell, c * PAD + r * 16 : c * PAD + r * 16 + 16, :]
                    place_rows(cell, c, ring, 0, 5, r, 5)
                    place_rows(cell, c, ring, 5, 3, 25 + r, 25)
                    place_rows(cell, c, ring, 8, 5, 100 + r, 5)
                    place_rows(cell, c, ring, 13, 3, 45 + r, 25)
                    place_rows(cell, c, planes[r], 0, 3, 30 + r, 5)
                    place_rows(cell, c, planes[r], 3, 3, 55 + r, 5)
                    place_rows(cell, c, planes[r], 6, 2, 80 + r, 5)
                place_rows(cell, c, tail, 0, 5, 90, 1)

    many(n - 1, 0).wait_send()
    for m in (0, 1):
        @pl.when(there(m))
        def _():
            strip_copy(xs, rx, m, 0, ()).wait_send()

    for m in (2, 3):
        @pl.when(there(m))
        def _():
            arriving(ys, ry, m, 0, ()).wait_recv()
            strip_copy(ys, ry, m, 0, ()).wait_send()
            arriving(es, re, m, 1, ()).wait_recv()
            strip_copy(es, re, m, 1, ()).wait_send()


def finish_kernel(cx, cy, pre, rx, ry, re, out_h, buf, out_sem):
    total = buf.shape[0]
    block = total // (cx * 3)
    rows_node = block // 125
    halves = rows_node // cy
    plane, quad = 25 * rows_node, 4 * halves
    line = (4 * cx - 1) * quad
    lane = lax.broadcasted_iota(jnp.int32, (quad, 128), 1)
    row = lax.broadcasted_iota(jnp.int32, (quad, 128), 0)
    copies, done = [], 0
    for k in range(cx * 3):
        x, c = k // 3, k % 3
        base = k * block
        buf[base : base + block, :] = pre[base : base + block, :]
        if x == 0:
            buf[base : base + plane, :] += rx[0, c, :plane]
        if x == cx - 1:
            buf[base + 4 * plane : base + 5 * plane, :] += rx[1, c, :plane]
        for side in (0, 1):
            tips = pltpu.roll(ry[side, 3 * line : 3 * line + quad, :], c, 1)
            ends = pltpu.roll(re[side, 6 * quad : 7 * quad, :], c, 1)
            for p in range(5):
                pp = x * 4 + p
                if pp % (4 * cx) == 0:
                    e = pp // (4 * cx)
                    at = (c * 2 + e) * quad
                    values, tip = re[side, at : at + quad, :], ends[e : e + 1]
                else:
                    at = c * line + (pp - 1) * quad
                    values, tip = ry[side, at : at + quad, :], tips[pp - 1 : pp]
                ahead = pltpu.roll(values, 127, 1)
                beyond = jnp.where(row == halves - 1, tip, pltpu.roll(ahead, quad - 1, 0))
                upper = jnp.where(lane < 127, ahead, beyond)
                to = base + (p * 25 + side * 20) * rows_node + side * (cy - 1)
                buf[pl.ds(to, quad, stride=cy), :] += values
                buf[pl.ds(to + quad * cy, halves, stride=cy), :] += upper[:halves]
        upto = (k + 1) * block // 8 * 8
        copy = pltpu.make_async_copy(
            buf.at[pl.ds(done, upto - done)], out_h.at[pl.ds(done, upto - done)], out_sem.at[k]
        )
        copy.start()
        copies.append(copy)
        done = upto
    for copy in copies:
        copy.wait()


def anywhere(count):
    return [pl.BlockSpec(memory_space=pl.ANY)] * count


def body(nx, ny, wavefield, moduli, residuals, coords, angles, element_ids, counts):
    cx, cy, depth = wavefield.shape[0], wavefield.shape[1], wavefield.shape[4]
    n, slots = nx * ny, residuals.shape[2]
    cells, halves = cx * cy, depth // 128
    span = min(n, SPAN)
    width = TILES * slots
    rows = wavefield.transpose(0, 2, 3, 1, 4).reshape(cx, 3, 125, cy, halves, 128)
    rows = rows.transpose(0, 1, 2, 4, 3, 5).reshape(-1, 128)
    coords = coords.transpose(0, 2, 1, 3)
    moduli = moduli.reshape(cells, 2, depth)
    operands = [residuals, coords, angles, element_ids, counts, rows, moduli, *tables()]
    quad = 4 * halves
    received = [
        (2, 3, -(-25 * halves * cy // 8) * 8, 128),
        (2, 3 * (4 * cx - 1) * quad + quad, 128),
        (2, 7 * quad, 128),
    ]
    scratch = [pltpu.VMEM(a.shape, a.dtype) for a in operands]
    scratch += [
        pltpu.VMEM((n, 8, slots), F32),
        pltpu.VMEM((n, 8, slots), F32),
        pltpu.VMEM((cells, 3 * PAD, depth), F32),
        pltpu.VMEM((6 * RING, width), BF16),
        pltpu.VMEM((6 * RING, width), BF16),
        pltpu.VMEM((6 * CORE, span * slots // 2), BF16),
        pltpu.VMEM((6 * CORE, span * slots // 2), BF16),
        pltpu.VMEM((span * slots // 2, cells * depth), BF16),
        pltpu.VMEM((span * slots // 2, cells * depth), BF16),
        pltpu.VMEM((cells, 3, PAD, depth), F32),
    ]
    scratch += [pltpu.VMEM(s, F32) for s in received + [(4, 3, quad, 128)]]
    scratch += [
        pltpu.SemaphoreType.DMA((len(operands),)),
        pltpu.SemaphoreType.DMA((1,)),
        pltpu.SemaphoreType.DMA((n // TILES,)),
        pltpu.SemaphoreType.DMA((6,)),
        pltpu.SemaphoreType.DMA((6,)),
    ]
    parts = pl.pallas_call(
        functools.partial(step_kernel, nx, ny, cx, cy),
        out_shape=[pltpu.VMEM(s, F32) for s in [rows.shape] + received],
        in_specs=anywhere(len(operands)),
        out_specs=[pl.BlockSpec(memory_space=pltpu.VMEM)] * 4,
        scratch_shapes=scratch,
        compiler_params=pltpu.CompilerParams(collective_id=0, has_side_effects=True, vmem_limit_bytes=48 << 20),
    )(*[pltpu.with_memory_space_constraint(a, pltpu.HBM) for a in operands])
    force = pl.pallas_call(
        functools.partial(finish_kernel, cx, cy),
        out_shape=jax.ShapeDtypeStruct(rows.shape, F32),
        in_specs=[pl.BlockSpec(memory_space=pltpu.VMEM)] * 4,
        out_specs=anywhere(1)[0],
        scratch_shapes=[pltpu.VMEM(rows.shape, F32), pltpu.SemaphoreType.DMA((cx * 3,))],
        compiler_params=pltpu.CompilerParams(vmem_limit_bytes=16 << 20),
    )(*parts)
    force = force.reshape(cx, 3, 125, halves, cy, 128).transpose(0, 1, 2, 4, 3, 5)
    return force.reshape(cx, 3, 125, cy, depth).transpose(0, 3, 1, 2, 4)


def solution(mesh):
    in_specs = (
        P("gx", "gy", None, None, None),
        P("gx", "gy", None, None),
        P(("gx", "gy"), None, None),
        P(("gx", "gy"), None, None, None),
        P(("gx", "gy"), None, None, None),
        P(("gx", "gy"), None, None),
        P(("gx", "gy"), None),
    )
    out_specs = P("gx", "gy", None, None, None)
    return jax.shard_map(
        functools.partial(body, mesh.shape["gx"], mesh.shape["gy"]),
        mesh=mesh,
        in_specs=in_specs,
        out_specs=out_specs,
        check_vma=False,
    )
```

```python
import functools
import math

import jax
import jax.numpy as jnp
import numpy as np
from jax import lax
from jax.experimental import pallas as pl
from jax.experimental.pallas import tpu as pltpu
from jax.sharding import PartitionSpec as P

MESH = pl.DeviceIdType.MESH
F32, BF16 = jnp.float32, jnp.bfloat16
PAD = 128
SPAN = 32
TILES = 4
RING, CORE = 80, 48

EDGE = [(0, 0), (0, 1), (0, 2), (0, 3), (0, 4), (1, 0), (2, 0), (3, 0)]
EDGE += [(4, 0), (4, 1), (4, 2), (4, 3), (4, 4), (1, 4), (2, 4), (3, 4)]
INNER = [(1, 1), (1, 2), (1, 3), (2, 1), (2, 2), (2, 3), (3, 1), (3, 2)]
LAST = (3, 3)


def node_order():
    order = []
    for r in range(5):
        order += [(p * 5 + q) * 5 + r for p, q in EDGE]
    for r in range(5):
        order += [(p * 5 + q) * 5 + r for p, q in INNER]
    order += [(LAST[0] * 5 + LAST[1]) * 5 + r for r in range(5)]
    return np.array(order)


def gll_points():
    return np.array([-1.0, -math.sqrt(3.0 / 7.0), 0.0, math.sqrt(3.0 / 7.0), 1.0])


def gll_weights():
    return np.array([0.1, 49.0 / 90.0, 32.0 / 45.0, 49.0 / 90.0, 0.1])


def derivative_table():
    points = gll_points()
    table = np.zeros((5, 5))
    for row in range(5):
        for col in range(5):
            if row == col:
                table[row, col] = sum(
                    (1.0 / (points[col] - points[other]) for other in range(5) if other != col)
                )
            else:
                value = 1.0 / (points[col] - points[row])
                for other in range(5):
                    if other != col and other != row:
                        value = (
                            value * (points[row] - points[other]) / (points[col] - points[other])
                        )
                table[row, col] = value
    return table


def split_table(table):
    high = table.astype(BF16)
    return high, (table - high.astype(np.float64)).astype(BF16)


def roots(k):
    points = gll_points()
    others = [m for m in range(5) if m != k]
    return [points[m] for m in others], 1.0 / np.prod([points[k] - points[m] for m in others])


def tables():
    dm, eye = derivative_table(), np.eye(5)
    w1 = gll_weights()
    weight = (w1[:, None, None] * w1[None, :, None] * w1[None, None, :]).reshape(-1)
    dirs = [
        np.kron(np.kron(dm, eye), eye),
        np.kron(np.kron(eye, dm), eye),
        np.kron(np.kron(eye, eye), dm),
    ]
    order = node_order()
    grad = np.zeros((3 * PAD, PAD))
    back = np.zeros((PAD, 3 * PAD))
    for j in range(3):
        grad[j * PAD : j * PAD + 125, :125] = dirs[j][order]
        full = -dirs[j].T * weight[None, :]
        back[:125, j * PAD : j * PAD + 125] = full[order][:, order]
    gh, gl = split_table(grad)
    bh, bl = split_table(back)
    g1 = np.concatenate([gh, gh], 1)
    bs = np.concatenate([bh, bl], 0)
    consts = np.zeros((41, 8, 128), np.float32)
    for g, group in enumerate((EDGE[:8], EDGE[8:], INNER, [LAST] * 8)):
        for row, (p, q) in enumerate(group):
            rp, sp = roots(p)
            rq, sq = roots(q)
            for j in range(4):
                consts[g * 9 + j, row] = rp[j]
                consts[g * 9 + 4 + j, row] = rq[j]
            consts[g * 9 + 8, row] = sp * sq
    for r in range(5):
        rr, sr = roots(r)
        for j in range(4):
            consts[36 + j, r] = rr[j]
        consts[40, r] = sr
    return jnp.asarray(g1), jnp.asarray(gl), jnp.asarray(bs), jnp.asarray(consts)


def split(x):
    high = x.astype(BF16)
    return high, (x - high.astype(F32)).astype(BF16)


def dot(a, b):
    return jnp.dot(a, b, preferred_element_type=F32)


def sin_cos(x):
    h = x * 0.5
    h2 = h * h
    s = c = None
    for k in range(6, -1, -1):
        a = (-1.0) ** k / math.factorial(2 * k + 1)
        b = (-1.0) ** k / math.factorial(2 * k)
        s = jnp.full(x.shape, a, F32) if s is None else s * h2 + a
        c = jnp.full(x.shape, b, F32) if c is None else c * h2 + b
    s = s * h
    return 2.0 * s * c, 1.0 - 2.0 * s * s


def quartic(x, rows):
    a, b, c, d = [x - row for row in rows]
    ab, cd = a * b, c * d
    return ab * cd, (a + b) * cd + ab * (c + d)


MOVES = [(-1, 0), (1, 0), (0, -1), (0, 1)]


def neighbour(m, gx, gy, nx, ny):
    step = MOVES[m][m // 2]
    pos, total = ((gx, nx), (gy, ny))[m // 2]
    return pos > 0 if step < 0 else pos < total - 1


def step_kernel(
    nx, ny, cx, cy, resid_h, coord_h, angle_h, ids_h, count_h, u_h, mod_h, g1_h, g2_h, bs_h,
    consts_h, pre_h, rx, ry, re,
    resid, coord, angle, ids, count, u_ref, mod_ref, g1, g2, bs, consts,
    packed, got, acc, lhs_a, lhs_b, in_a, in_b, hot_a, hot_b, pad, xs, ys, es, tips,
    load_sem, send_sem, recv_sem, halo_send, halo_recv,
):
    n = nx * ny
    gx, gy = lax.axis_index("gx"), lax.axis_index("gy")
    me = gx * ny + gy
    cells, depth, slots = cx * cy, acc.shape[2], resid.shape[2]
    halves = depth // 128
    rows_node = halves * cy
    span = min(n, SPAN)
    chunks = span // TILES
    width = TILES * slots
    barrier = pltpu.get_barrier_semaphore()

    def after(k):
        to = me + k
        to = jnp.where(to >= n, to - n, to)
        return to, (lax.div(to, ny), lax.rem(to, ny))

    def greet(k):
        pl.semaphore_signal(barrier, inc=1, device_id=after(k)[1], device_id_type=MESH)

    def repeat(action):
        if n <= SPAN:
            for k in range(1, n):
                action(k)
        else:
            def one(k, c):
                action(k)
                return c

            lax.fori_loop(1, n, one, 0)

    pairs = [
        (count_h, count), (angle_h, angle), (resid_h, resid), (coord_h, coord), (ids_h, ids),
        (u_h, u_ref), (mod_h, mod_ref), (g1_h, g1), (g2_h, g2), (bs_h, bs), (consts_h, consts),
    ]
    loads = [pltpu.make_async_copy(a, b, load_sem.at[k]) for k, (a, b) in enumerate(pairs)]
    for copy in loads:
        copy.start()
    repeat(greet)
    for copy in loads[:5]:
        copy.wait()

    rows = lax.broadcasted_iota(jnp.int32, (n, n), 0)
    cols = lax.broadcasted_iota(jnp.int32, (n, n), 1)
    diagonal = jnp.where(rows == cols, count[...].astype(F32), 0.0)
    live_count = jnp.sum(diagonal, axis=1, keepdims=True)
    slot = lax.broadcasted_iota(jnp.int32, (n, slots), 1).astype(F32)
    sa, ca = sin_cos(angle[0, :, 0, :])
    sd, cd = sin_cos(angle[0, :, 1, :])
    packed[:, 0, :] = jnp.where(slot < live_count, resid[0], 0.0)
    for d in range(3):
        packed[:, 1 + d, :] = coord[0, d]
    packed[:, 4, :] = ca * cd
    packed[:, 5, :] = sa * cd
    packed[:, 6, :] = sd
    packed[:, 7, :] = ids[0].astype(F32)
    tips[...] = jnp.zeros_like(tips)
    for m in range(4):
        @pl.when(jnp.logical_not(neighbour(m, gx, gy, nx, ny)))
        def _():
            for hole in ((rx,), (ry, re))[m // 2]:
                hole[m % 2] = jnp.zeros(hole.shape[1:], F32)

    def strain(cell, slab, c):
        start = ((cell // cy) * 3 + c) * 125 * rows_node + cell % cy
        for h in range(halves):
            pad[slab, c, 0:125, h * 128 : (h + 1) * 128] = u_ref[
                pl.ds(start + h * cy, 125, stride=rows_node), :
            ]
        high, low = split(pad[slab, c])
        r = dot(g1[...], jnp.concatenate([high, low], axis=0)) + dot(g2[...], high)
        return [r[j * PAD : (j + 1) * PAD] for j in range(3)]

    def stiff(group):
        g = {cell: [] for cell in group}
        for c in range(3):
            for cell in group:
                g[cell].append(strain(cell, cell % len(group), c))
        press = {}
        for cell in group:
            press[cell] = mod_ref[cell, 0:1, :] * (g[cell][0][0] + g[cell][1][1] + g[cell][2][2])
        for i in range(3):
            for cell in group:
                mu, parts = mod_ref[cell, 1:2, :], []
                for j in range(3):
                    s = mu * (g[cell][i][j] + g[cell][j][i])
                    parts.append(s + press[cell] if i == j else s)
                high, low = split(jnp.concatenate(parts, axis=0))
                r = dot(bs[...], high)
                acc[cell, i * PAD : (i + 1) * PAD, :] = r[:PAD] + r[PAD:] + dot(bs[:PAD], low)

    pl.semaphore_wait(barrier, n - 1)

    def tile_copy(k, at):
        to, where = after(k)
        return pltpu.make_async_remote_copy(
            src_ref=packed.at[to],
            dst_ref=got.at[at],
            send_sem=send_sem.at[0],
            recv_sem=recv_sem.at[(k - 1) // TILES],
            device_id=where,
            device_id_type=MESH,
        )

    def send(k):
        tile_copy(k, me).start()

    repeat(send)
    got[me] = packed[me]
    pad[:, :, PAD - 8 :, :] = jnp.zeros((cells, 3, 8, depth), F32)
    for copy in loads[5:]:
        copy.wait()
    stiff(range(cells))

    def many(count, group):
        other = lax.rem(me + 1, n)
        return pltpu.make_async_remote_copy(
            src_ref=packed.at[pl.ds(0, count)],
            dst_ref=got.at[pl.ds(0, count)],
            send_sem=send_sem.at[0],
            recv_sem=recv_sem.at[group],
            device_id=(other // ny, lax.rem(other, ny)),
            device_id_type=MESH,
        )

    def wait_tiles(first, count):
        many(count, (first - 1) // TILES).wait_recv()

    def prepare(first, ring, inner, hot, at):
        tiles = [got[lax.rem(me - (first + i) + n, n)] for i in range(TILES)]
        tile = jnp.concatenate(tiles, axis=1)

        def const(k):
            return jnp.concatenate([consts[k]] * TILES, axis=1)

        v = tile[0:1]
        t = [tile[4 + i : 5 + i] for i in range(3)]
        x, y, z = [jnp.broadcast_to(tile[1 + d : 2 + d], (8, width)) for d in range(3)]
        lz, dz = quartic(z, [const(36 + j) for j in range(4)])
        lz, dz = lz * const(40), dz * (const(40) * t[2])
        first_of, second_of = [], []
        for g in range(4):
            lx, dx = quartic(x, [const(g * 9 + j) for j in range(4)])
            ly, dy = quartic(y, [const(g * 9 + 4 + j) for j in range(4)])
            scale = const(g * 9 + 8)
            first_of.append(scale * ((t[0] * dx) * ly + (t[1] * dy) * lx))
            second_of.append(scale * (lx * ly))
        edge, core = [], []
        for r in range(5):
            a = jnp.broadcast_to(lz[r : r + 1], (8, width))
            b = jnp.broadcast_to(dz[r : r + 1], (8, width))
            edge += [first_of[g] * a + second_of[g] * b for g in (0, 1)]
            core.append(first_of[2] * a + second_of[2] * b)
        core.append(first_of[3] * lz + second_of[3] * dz)
        edge, core = jnp.concatenate(edge, axis=0), jnp.concatenate(core, axis=0)
        for i in range(3):
            w = v * t[i]
            high, low = split(edge * w)
            ring[2 * i * RING : (2 * i + 1) * RING, :] = high
            ring[(2 * i + 1) * RING : (2 * i + 2) * RING, :] = low
            high, low = split(core * w)
            inner[2 * i * CORE : (2 * i + 1) * CORE, pl.ds(at, width)] = high
            inner[(2 * i + 1) * CORE : (2 * i + 2) * CORE, pl.ds(at, width)] = low
        number = lax.broadcasted_iota(jnp.int32, (slots, cells * depth), 1).astype(F32)
        for i in range(TILES):
            ident = tiles[i].T[:, 7:8]
            hot[pl.ds(at + i * slots, slots), :] = jnp.where(number == ident, 1.0, 0.0).astype(BF16)

    def gather_ring(ring, hot, at):
        for cell in range(cells):
            r = dot(ring[...], hot[pl.ds(at, width), cell * depth : (cell + 1) * depth])
            for i in range(3):
                acc[cell, i * PAD : i * PAD + RING, :] += (
                    r[2 * i * RING : (2 * i + 1) * RING]
                    + r[(2 * i + 1) * RING : (2 * i + 2) * RING]
                )

    def gather_core(cell):
        where = slice(cell * depth, (cell + 1) * depth)
        r = dot(in_a[...], hot_a[:, where]) + dot(in_b[...], hot_b[:, where])
        return [
            acc[cell, i * PAD + RING : (i + 1) * PAD, :]
            + r[2 * i * CORE : (2 * i + 1) * CORE]
            + r[(2 * i + 1) * CORE : (2 * i + 2) * CORE]
            for i in range(3)
        ]

    def inject(first, last):
        wait_tiles(first, TILES)
        prepare(first, lhs_a, in_a, hot_a, 0)

        def pair(j, carry):
            one, two = first + (2 * j + 1) * TILES, first + (2 * j + 2) * TILES
            wait_tiles(one, TILES)
            here = pl.multiple_of(j * width, width)
            then = pl.multiple_of((j + 1) * width, width)
            prepare(one, lhs_b, in_b, hot_b, here)
            gather_ring(lhs_a, hot_a, here)
            wait_tiles(two, TILES)
            prepare(two, lhs_a, in_a, hot_a, then)
            gather_ring(lhs_b, hot_b, here)
            return carry

        half = chunks // 2
        lax.fori_loop(0, half - 1, pair, 0)
        end = first + (chunks - 1) * TILES
        wait_tiles(end, TILES - 1 if last else TILES)
        prepare(end, lhs_b, in_b, hot_b, (half - 1) * width)
        gather_ring(lhs_a, hot_a, (half - 1) * width)
        gather_ring(lhs_b, hot_b, (half - 1) * width)

    if n > span:
        def early(b, carry):
            inject(b * span + 1, False)
            for cell in range(cells):
                for i, f in enumerate(gather_core(cell)):
                    acc[cell, i * PAD + RING : (i + 1) * PAD, :] = f
            return carry

        lax.fori_loop(0, n // span - 1, early, 0)
    inject(n - span + 1, True)

    def stitch(low, high):
        lane = lax.broadcasted_iota(jnp.int32, low.shape, 1)
        up = jnp.where(lane < depth - 1, pltpu.roll(low, depth - 1, 1), 0.0)
        down = jnp.where(lane > 0, pltpu.roll(high, 1, 1), 0.0)
        return low + down, high + up

    def join(a, ra, b, rb, size):
        total = acc[a, ra : ra + size, :] + acc[b, rb : rb + size, :]
        acc[a, ra : ra + size, :] = total
        acc[b, rb : rb + size, :] = total

    def there(m):
        return neighbour(m, gx, gy, nx, ny)

    quad = 4 * halves
    line = (4 * cx - 1) * quad
    last = slice(depth - 128, depth)

    def strip_copy(src, dst, m, slot, where):
        dx, dy = MOVES[m]
        side, other = m % 2, 1 - m % 2
        return pltpu.make_async_remote_copy(
            src_ref=src.at[(side,) + where],
            dst_ref=dst.at[(other,) + where],
            send_sem=halo_send.at[2 * slot + m],
            recv_sem=halo_recv.at[2 * slot + m],
            device_id=(gx + dx, gy + dy),
            device_id_type=MESH,
        )

    def arriving(src, dst, m, slot, where):
        dx, dy = MOVES[m]
        return pltpu.make_async_remote_copy(
            src_ref=src.at[(m % 2,) + where],
            dst_ref=dst.at[(m % 2,) + where],
            send_sem=halo_send.at[2 * slot + m],
            recv_sem=halo_recv.at[2 * slot + m + 1 - 2 * (m % 2)],
            device_id=(gx + dx, gy + dy),
            device_id_type=MESH,
        )

    def part(c):
        return (pl.ds(c * line, line + (quad if c == 2 else 0)),)

    def pack_tips(rows):
        lane = lax.broadcasted_iota(jnp.int32, rows[0].shape, 1)
        total = rows[0]
        for c in (1, 2):
            total = jnp.where(lane == 127 - c, pltpu.roll(rows[c], 128 - c, 1), total)
        return total

    for c in range(3):
        o = c * PAD
        for cell in range(cells):
            low, high = stitch(acc[cell, o : o + 16, :], acc[cell, o + 64 : o + 80, :])
            acc[cell, o : o + 16, :] = low
            acc[cell, o + 64 : o + 80, :] = high
        for r in range(5):
            k = o + r * 16
            for y in range(cy):
                for x in range(cx - 1):
                    join(x * cy + y, k + 8, (x + 1) * cy + y, k, 5)
            for x in range(cx):
                for y in range(cy - 1):
                    a, b = x * cy + y, x * cy + y + 1
                    join(a, k + 13, b, k + 5, 3)
                    join(a, k + 4, b, k, 1)
                    join(a, k + 12, b, k + 8, 1)
        for side in (0, 1):
            low, mid, high = ((0, 5, 8), (4, 13, 12))[side]
            for x in range(cx):
                cell = x * cy + side * (cy - 1)
                for r in range(4):
                    k = o + r * 16
                    for h in range(halves):
                        lanes = slice(h * 128, (h + 1) * 128)
                        to = r * halves + h
                        at = c * line + x * 4 * quad + to
                        ys[side, pl.ds(at, 3, stride=quad), :] = acc[
                            cell, k + mid : k + mid + 3, lanes
                        ]
                        if x < cx - 1:
                            ys[side, at + 3 * quad : at + 3 * quad + 1, :] = acc[
                                cell, k + high : k + high + 1, lanes
                            ]
                        for e, row in ((0, low), (1, high)):
                            if x == e * (cx - 1):
                                at_e = (c * 2 + e) * quad + to
                                es[side, at_e : at_e + 1, :] = acc[
                                    cell, k + row : k + row + 1, lanes
                                ]
                k = o + 64
                tips[side, c, x * 4 : x * 4 + 3, :] = acc[cell, k + mid : k + mid + 3, last]
                for e, row in ((0, low), (1, high)):
                    if x == e * (cx - 1):
                        tips[2 + side, c, e : e + 1, :] = acc[cell, k + row : k + row + 1, last]
                if x < cx - 1:
                    tips[side, c, x * 4 + 3 : x * 4 + 4, :] = acc[cell, k + high : k + high + 1, last]
            if c == 2:
                ys[side, 3 * line : 3 * line + quad, :] = pack_tips([tips[side, d] for d in range(3)])
        for m in (2, 3):
            @pl.when(there(m))
            def _():
                strip_copy(ys, ry, m, 0, part(c)).start()
        for y in range(cy):
            for side in (0, 1):
                cell = side * (cx - 1) * cy + y
                for h in range(halves):
                    for r in range(5):
                        k = o + r * 16 + side * 8
                        xs[side, c, pl.ds(r * rows_node + h * cy + y, 5, stride=5 * rows_node), :] = (
                            acc[cell, k : k + 5, h * 128 : (h + 1) * 128]
                        )
        for m in (0, 1):
            @pl.when(there(m))
            def _():
                strip_copy(xs, rx, m, 0, (c,)).start()

    def place_rows(cell, c, values, row, size, node, step):
        start = ((cell // cy) * 3 + c) * 125 * rows_node + cell % cy
        for h in range(halves):
            at = start + h * cy + node * rows_node
            part = values[row : row + size, h * 128 : (h + 1) * 128]
            pre_h[pl.ds(at, size, stride=step * rows_node), :] = part

    def fold_edges():
        for m in (0, 1):
            @pl.when(there(m))
            def _():
                arriving(xs, rx, m, 0, ()).wait_recv()
                for c in range(3):
                    for side in (0, 1):
                        at = side * (20 * rows_node + cy - 1)
                        k = (c * 2 + m) * quad
                        es[side, k : k + quad, :] += rx[m, c, pl.ds(at, quad, stride=cy), :]
                        tip = at + 4 * rows_node + (halves - 1) * cy
                        tips[2 + side, c, m : m + 1, :] += rx[m, c, tip : tip + 1, :]

        for side in (0, 1):
            es[side, 6 * quad : 7 * quad, :] = pack_tips([tips[2 + side, d] for d in range(3)])
            m = 2 + side

            @pl.when(there(m))
            def _():
                strip_copy(es, re, m, 1, ()).start()

    for x in range(cx):
        for y in range(cy):
            cell = x * cy + y
            if cell == 1:
                fold_edges()
            inner = gather_core(cell)
            for c in range(3):
                f = inner[c]
                low, high = stitch(f[0:8], f[32:40])
                lane = lax.broadcasted_iota(jnp.int32, (8, depth), 1)
                row = lax.broadcasted_iota(jnp.int32, (8, depth), 0)
                tail = f[40:48]
                up = pltpu.roll(pltpu.roll(tail, depth - 1, 1), 4, 0)
                down = pltpu.roll(pltpu.roll(tail, 1, 1), 4, 0)
                tail = (
                    tail
                    + jnp.where((row == 4) & (lane < depth - 1), up, 0.0)
                    + jnp.where((row == 0) & (lane > 0), down, 0.0)
                )
                planes = [low, f[8:16], f[16:24], f[24:32], high]
                for r in range(5):
                    ring = acc[cell, c * PAD + r * 16 : c * PAD + r * 16 + 16, :]
                    place_rows(cell, c, ring, 0, 5, r, 5)
                    place_rows(cell, c, ring, 5, 3, 25 + r, 25)
                    place_rows(cell, c, ring, 8, 5, 100 + r, 5)
                    place_rows(cell, c, ring, 13, 3, 45 + r, 25)
                    place_rows(cell, c, planes[r], 0, 3, 30 + r, 5)
                    place_rows(cell, c, planes[r], 3, 3, 55 + r, 5)
                    place_rows(cell, c, planes[r], 6, 2, 80 + r, 5)
                place_rows(cell, c, tail, 0, 5, 90, 1)

    many(n - 1, 0).wait_send()
    for m in (0, 1):
        @pl.when(there(m))
        def _():
            strip_copy(xs, rx, m, 0, ()).wait_send()

    for m in (2, 3):
        @pl.when(there(m))
        def _():
            arriving(ys, ry, m, 0, ()).wait_recv()
            strip_copy(ys, ry, m, 0, ()).wait_send()
            arriving(es, re, m, 1, ()).wait_recv()
            strip_copy(es, re, m, 1, ()).wait_send()


def finish_kernel(cx, cy, pre, rx, ry, re, out_h, buf, out_sem):
    total = buf.shape[0]
    block = total // (cx * 3)
    rows_node = block // 125
    halves = rows_node // cy
    plane, quad = 25 * rows_node, 4 * halves
    line = (4 * cx - 1) * quad
    lane = lax.broadcasted_iota(jnp.int32, (quad, 128), 1)
    row = lax.broadcasted_iota(jnp.int32, (quad, 128), 0)
    copies, done = [], 0
    for k in range(cx * 3):
        x, c = k // 3, k % 3
        base = k * block
        buf[base : base + block, :] = pre[base : base + block, :]
        if x == 0:
            buf[base : base + plane, :] += rx[0, c, :plane]
        if x == cx - 1:
            buf[base + 4 * plane : base + 5 * plane, :] += rx[1, c, :plane]
        for side in (0, 1):
            tips = pltpu.roll(ry[side, 3 * line : 3 * line + quad, :], c, 1)
            ends = pltpu.roll(re[side, 6 * quad : 7 * quad, :], c, 1)
            for p in range(5):
                pp = x * 4 + p
                if pp % (4 * cx) == 0:
                    e = pp // (4 * cx)
                    at = (c * 2 + e) * quad
                    values, tip = re[side, at : at + quad, :], ends[e : e + 1]
                else:
                    at = c * line + (pp - 1) * quad
                    values, tip = ry[side, at : at + quad, :], tips[pp - 1 : pp]
                ahead = pltpu.roll(values, 127, 1)
                beyond = jnp.where(row == halves - 1, tip, pltpu.roll(ahead, quad - 1, 0))
                upper = jnp.where(lane < 127, ahead, beyond)
                to = base + (p * 25 + side * 20) * rows_node + side * (cy - 1)
                buf[pl.ds(to, quad, stride=cy), :] += values
                buf[pl.ds(to + quad * cy, halves, stride=cy), :] += upper[:halves]
        upto = (k + 1) * block // 8 * 8
        copy = pltpu.make_async_copy(
            buf.at[pl.ds(done, upto - done)], out_h.at[pl.ds(done, upto - done)], out_sem.at[k]
        )
        copy.start()
        copies.append(copy)
        done = upto
    for copy in copies:
        copy.wait()


def anywhere(count):
    return [pl.BlockSpec(memory_space=pl.ANY)] * count


def body(nx, ny, wavefield, moduli, residuals, coords, angles, element_ids, counts):
    cx, cy, depth = wavefield.shape[0], wavefield.shape[1], wavefield.shape[4]
    n, slots = nx * ny, residuals.shape[2]
    cells, halves = cx * cy, depth // 128
    span = min(n, SPAN)
    width = TILES * slots
    rows = wavefield.transpose(0, 2, 3, 1, 4).reshape(cx, 3, 125, cy, halves, 128)
    rows = rows.transpose(0, 1, 2, 4, 3, 5).reshape(-1, 128)
    coords = coords.transpose(0, 2, 1, 3)
    moduli = moduli.reshape(cells, 2, depth)
    operands = [residuals, coords, angles, element_ids, counts, rows, moduli, *tables()]
    quad = 4 * halves
    received = [
        (2, 3, -(-25 * halves * cy // 8) * 8, 128),
        (2, 3 * (4 * cx - 1) * quad + quad, 128),
        (2, 7 * quad, 128),
    ]
    scratch = [pltpu.VMEM(a.shape, a.dtype) for a in operands]
    scratch += [
        pltpu.VMEM((n, 8, slots), F32),
        pltpu.VMEM((n, 8, slots), F32),
        pltpu.VMEM((cells, 3 * PAD, depth), F32),
        pltpu.VMEM((6 * RING, width), BF16),
        pltpu.VMEM((6 * RING, width), BF16),
        pltpu.VMEM((6 * CORE, span * slots // 2), BF16),
        pltpu.VMEM((6 * CORE, span * slots // 2), BF16),
        pltpu.VMEM((span * slots // 2, cells * depth), BF16),
        pltpu.VMEM((span * slots // 2, cells * depth), BF16),
        pltpu.VMEM((cells, 3, PAD, depth), F32),
    ]
    scratch += [pltpu.VMEM(s, F32) for s in received + [(4, 3, quad, 128)]]
    scratch += [
        pltpu.SemaphoreType.DMA((len(operands),)),
        pltpu.SemaphoreType.DMA((1,)),
        pltpu.SemaphoreType.DMA((n // TILES,)),
        pltpu.SemaphoreType.DMA((6,)),
        pltpu.SemaphoreType.DMA((6,)),
    ]
    parts = pl.pallas_call(
        functools.partial(step_kernel, nx, ny, cx, cy),
        out_shape=[pltpu.VMEM(s, F32) for s in [rows.shape] + received],
        in_specs=anywhere(len(operands)),
        out_specs=[pl.BlockSpec(memory_space=pltpu.VMEM)] * 4,
        scratch_shapes=scratch,
        compiler_params=pltpu.CompilerParams(collective_id=0, has_side_effects=True, vmem_limit_bytes=48 << 20),
    )(*[pltpu.with_memory_space_constraint(a, pltpu.HBM) for a in operands])
    force = pl.pallas_call(
        functools.partial(finish_kernel, cx, cy),
        out_shape=jax.ShapeDtypeStruct(rows.shape, F32),
        in_specs=[pl.BlockSpec(memory_space=pltpu.VMEM)] * 4,
        out_specs=anywhere(1)[0],
        scratch_shapes=[pltpu.VMEM(rows.shape, F32), pltpu.SemaphoreType.DMA((cx * 3,))],
        compiler_params=pltpu.CompilerParams(vmem_limit_bytes=16 << 20),
    )(*parts)
    force = force.reshape(cx, 3, 125, halves, cy, 128).transpose(0, 1, 2, 4, 3, 5)
    return force.reshape(cx, 3, 125, cy, depth).transpose(0, 3, 1, 2, 4)


def solution(mesh):
    in_specs = (
        P("gx", "gy", None, None, None),
        P("gx", "gy", None, None),
        P(("gx", "gy"), None, None),
        P(("gx", "gy"), None, None, None),
        P(("gx", "gy"), None, None, None),
        P(("gx", "gy"), None, None),
        P(("gx", "gy"), None),
    )
    out_specs = P("gx", "gy", None, None, None)
    return jax.shard_map(
        functools.partial(body, mesh.shape["gx"], mesh.shape["gy"]),
        mesh=mesh,
        in_specs=in_specs,
        out_specs=out_specs,
        check_vma=False,
    )
```
